256 devices in a mesh: row: 16 (over y, x_hi, core), col: 16 (over x_lo, z).
Axes of the slice: x: 4 (x_hi: 2, x_lo: 2; x = x_hi * 2 + x_lo), y: 4, z: 8, core: 2. Of those that a mesh axis runs over, the one named last changes fastest.
Arguments:
- grad_out: bfloat16 [512, 512, 320], P('row', 'col'), may hold values from -0.0390625 to 0.0390625
- dec_pre: bfloat16 [512, 512, 320], P('row', 'col'), may hold values from -6 to 6
- ctrl_out: bfloat16 [512, 512, 320], P('row', 'col'), may hold values from -6 to 6
- ctrl_mid: bfloat16 [512, 512, 320], P('row', 'col'), may hold values from -6 to 6
- ctrl_in: bfloat16 [512, 512, 320], P('row', 'col'), may hold values from -6 to 6
- dec_weight: bfloat16 [3, 3, 320, 320], replicated, may hold values from -0.109375 to 0.109375
- zero_weight: bfloat16 [320, 320], replicated, may hold values from -0.3125 to 0.3125
- ctrl_weight: bfloat16 [3, 3, 320, 320], replicated, may hold values from -0.109375 to 0.109375
Outputs:
- grad_zero: float32 [320, 320], P('row', 'col')
- grad_ctrl: float32 [3, 3, 320, 320], P(None, None, 'row', 'col')
- grad_in: float32 [3, 3, 320, 320], P(None, None, 'row', 'col')
The draws below stay inside these ranges and needn't reach their ends.
All inputs are finite; a program needn't handle non-finite values.
Results may differ from the reference program's by a relative error of at most 0.024.
Values may be sent and summed in bfloat16 or wider, within the bound.
A program may use at most 128 MiB of HBM per device.

```python
import jax
import jax.numpy as jnp
from jax import lax

C = 320
TH = 32
NH = 512
NW = 512
N_ROW = 16


def raised(values, rng, source, target, shards_of, factor):
    def block_of(position):
        return (jnp.arange(values.shape[position]) // (values.shape[position] // shards_of)).reshape((-1,) + (1,) * (values.ndim - 1 - position))

    near = jax.random.permutation(rng, shards_of)[block_of(target)]
    other_side = (block_of(target) + shards_of // 2) % shards_of
    return jnp.where((block_of(source) == near) | (block_of(source) == other_side), factor * values, values)


def block_scale(key, dims, split, least, largest):
    level = 1.0
    for dim, parts in split:
        heights = jax.random.uniform(jax.random.fold_in(jax.random.fold_in(key, 6), dim), (parts,), jnp.float32, least / len(split), largest / len(split))
        level = level * jnp.repeat(jnp.exp(heights), dims[dim] // parts).reshape((-1,) + (1,) * (len(dims) - 1 - dim))
    return level


def centred(rng, dims, scale, most, pieces=(), kind=jnp.bfloat16):
    gain = block_scale(rng, dims, pieces, -0.22, 0.18) if pieces else 1.0
    entries = jax.random.normal(rng, dims, jnp.float32) * scale * gain
    return jnp.minimum(jnp.maximum(entries, -most), most).astype(kind)


def bell_draw_with(own_key, extent, width, reach, pieces, heavy, kind=jnp.bfloat16):
    entries = width * jax.random.normal(own_key, extent, jnp.float32)
    if pieces:
        entries = entries * block_scale(own_key, extent, pieces, -0.22, 0.18)
    return jnp.clip(raised(entries, jax.random.fold_in(own_key, 3), *heavy), -reach, reach).astype(kind)


def setup_inputs(seed: int = 0) -> dict:
    key_of = jax.random.split(jax.random.key(seed), 9)
    grad_out = bell_draw_with(key_of[0], (NH, NW, C), (1.0 / (TH * N_ROW)), 0.0390625, ((0, 16), (1, 16)), (0, 2, 16, 2.0))
    dec_pre = centred(key_of[1], (NH, NW, C), 1.0, 6.0, ((0, 16), (1, 16)))
    ctrl_out = bell_draw_with(key_of[2], (NH, NW, C), 1.0, 6.0, ((0, 16), (1, 16)), (1, 2, 16, 2.0))
    ctrl_mid = centred(key_of[3], (NH, NW, C), 1.0, 6.0, ((0, 16), (1, 16)))
    ctrl_in = bell_draw_with(key_of[4], (NH, NW, C), 1.0, 6.0, ((0, 16), (1, 16)), (0, 2, 16, 2.0))
    dec_weight = centred(key_of[5], (3, 3, C, C), (9 * C) ** -0.5, 0.109375)
    zero_weight = centred(key_of[6], (C, C), C ** -0.5, 0.3125)
    ctrl_weight = centred(key_of[7], (3, 3, C, C), (9 * C) ** -0.5, 0.109375)
    return dict(grad_out=grad_out, dec_pre=dec_pre, ctrl_out=ctrl_out, ctrl_mid=ctrl_mid, ctrl_in=ctrl_in, dec_weight=dec_weight, zero_weight=zero_weight, ctrl_weight=ctrl_weight)


def silu_slope(values):
    sigm = jax.nn.sigmoid(values)
    return sigm * (1.0 + values * (1.0 - sigm))

def transpose_conv(cotangent, kernel):
    height, breadth, channels = cotangent.shape
    padded = jnp.pad(cotangent, ((1, 1), (1, 1), (0, 0)))
    summed = jnp.zeros((height * breadth, channels), jnp.float32)
    for tap_row in range(3):
        for tap_col in range(3):
            window = padded[2 - tap_row:2 - tap_row + height, 2 - tap_col:2 - tap_col + breadth].reshape(-1, channels)
            summed = summed + jnp.dot(window, kernel[tap_row, tap_col].T, preferred_element_type=jnp.float32)
    return summed.reshape(height, breadth, channels)

def weight_grad(activation, cotangent):
    height, breadth, channels = cotangent.shape
    padded = jnp.pad(activation, ((1, 1), (1, 1), (0, 0)))
    flat_grad = cotangent.reshape(-1, channels)
    taps = []
    for tap_row in range(3):
        for tap_col in range(3):
            window = padded[tap_row:tap_row + height, tap_col:tap_col + breadth].reshape(-1, channels)
            taps.append(lax.dot_general(window, flat_grad, (((0,), (0,)), ((), ())), preferred_element_type=jnp.float32))
    return jnp.stack(taps).reshape(3, 3, channels, channels)

def reference(grad_out, dec_pre, ctrl_out, ctrl_mid, ctrl_in, dec_weight, zero_weight, ctrl_weight):
    height, breadth, channels = grad_out.shape
    dec_grad = (silu_slope(dec_pre.astype(jnp.float32)) * transpose_conv(grad_out, dec_weight)).astype(jnp.bfloat16)
    flat_dec = dec_grad.reshape(-1, channels)
    grad_zero = lax.dot_general(ctrl_out.reshape(-1, channels), flat_dec, (((0,), (0,)), ((), ())), preferred_element_type=jnp.float32)
    ctrl_grad = jnp.dot(flat_dec, zero_weight.T, preferred_element_type=jnp.float32).astype(jnp.bfloat16).reshape(height, breadth, channels)
    mid_grad = (silu_slope(ctrl_mid.astype(jnp.float32)) * transpose_conv(ctrl_grad, ctrl_weight)).astype(jnp.bfloat16)
    act_mid = jax.nn.silu(ctrl_mid.astype(jnp.float32)).astype(jnp.bfloat16)
    act_in = jax.nn.silu(ctrl_in.astype(jnp.float32)).astype(jnp.bfloat16)
    grad_ctrl = weight_grad(act_mid, ctrl_grad)
    grad_in = weight_grad(act_in, mid_grad)
    return (grad_zero, grad_ctrl, grad_in)
```

```python
import functools

import jax
import jax.numpy as jnp
import numpy as np
from jax import lax
from jax.experimental import pallas as pl
from jax.experimental.pallas import tpu as pltpu
from jax.sharding import PartitionSpec as P

F32 = jnp.float32
BF16 = jnp.bfloat16
MESH = pl.DeviceIdType.MESH
NT = (((1,), (1,)), ((), ()))
NN = (((1,), (0,)), ((), ()))
C = 320
T = 32
ROWS_A, SPLIT_A, ZA = 320, 160, 48
ROWS_B, SPLIT_B, ZB = 240, 128, 32


def dot(a, b, dims=NN):
    return lax.dot_general(a, b, dims, preferred_element_type=F32)


def silu(v):
    return v * jax.nn.sigmoid(v)


def slope(v):
    s = jax.nn.sigmoid(v)
    return s * (1.0 + v * (1.0 - s))


def tables():
    place = np.full((16, 256), -1, np.int32)
    for y in range(4):
        for s in range(3):
            for xh in range(2):
                for core in range(2):
                    for c in range(20):
                        lane = xh * 128 + core * 64 + s * 20 + c
                        place[y * 3 + s, lane] = y * 80 + xh * 40 + core * 20 + c - (128 if y == 3 else 0)
    order = np.zeros((C, 1), np.int32)
    for core in range(2):
        for xl in range(2):
            for z in range(8):
                for i in range(10):
                    order[core * 160 + xl * 80 + z * 10 + i, 0] = (xl * 8 + z) * 20 + core * 10 + i
    za = np.full((8 * ZA, 1), -1, np.int32)
    zb = np.full((8 * ZB, 1), -1, np.int32)
    for z in range(8):
        for g in range(4):
            for i in range(10):
                za[z * ZA + g * 10 + i, 0] = g * 80 + z * 10 + i
                if g < 3:
                    zb[z * ZB + g * 10 + i, 0] = g * 80 + z * 10 + i
    return place, order, za, zb


def kernel(
    g_hbm, pre_hbm, cout_hbm, mid_hbm, cin_hbm, wd_hbm, wz_hbm, wc_hbm,
    place_ref, order_ref, za_ref, zb_ref,
    out_a, out_b,
    in4, pre, cout, wd, wz, wc,
    scol, hrow, hcol, hcor, hc32,
    sh, rem, wrem, dec, xmid, xin, xout, pmat, omat, gt, mgrad,
    ra, ca, ya, xa, ea, fa, ya2, xa2, da, zsa, zra, fina, pina,
    rb, cb, yb, xb, eb, fb, yb2, xb2, db, zsb, zrb, finb, pinb,
    load_sem, hs_sem, hr_sem, cs_sem, cr_sem, ss_sem, sr_sem,
):
    row = lax.axis_index("row")
    col = lax.axis_index("col")
    y, xh, core = row // 4, (row // 2) % 2, row % 2
    xl, z = col // 8, col % 8
    x = xh * 2 + xl

    def at_y(t):
        return ((t * 2 + xh) * 2 + core, col)

    def at_x(t):
        return ((y * 2 + t // 2) * 2 + core, (t % 2) * 8 + z)

    def at_z(t):
        return (row, xl * 8 + t)

    partner = (row + 1 - 2 * core, col)

    loads = [
        pltpu.make_async_copy(g_hbm, in4.at[0], load_sem.at[0]),
        pltpu.make_async_copy(mid_hbm, in4.at[1], load_sem.at[1]),
        pltpu.make_async_copy(cin_hbm, in4.at[2], load_sem.at[2]),
        pltpu.make_async_copy(wd_hbm, wd, load_sem.at[3]),
        pltpu.make_async_copy(pre_hbm, pre, load_sem.at[4]),
        pltpu.make_async_copy(wz_hbm, wz, load_sem.at[5]),
        pltpu.make_async_copy(cout_hbm, cout, load_sem.at[6]),
        pltpu.make_async_copy(wc_hbm, wc, load_sem.at[7]),
    ]
    for copy in loads:
        copy.start()

    has = {-1: (row > 0, col > 0), 1: (row < 15, col < 15), 0: (row >= 0, col >= 0)}
    around = [(dr, dc) for dr in (-1, 0, 1) for dc in (-1, 0, 1) if (dr, dc) != (0, 0)]
    there = {d: jnp.logical_and(has[d[0]][0], has[d[1]][1]) for d in around}

    barrier = pltpu.get_barrier_semaphore()
    for d in around:
        @pl.when(there[d])
        def _(d=d):
            pl.semaphore_signal(barrier, inc=1, device_id=(row + d[0], col + d[1]), device_id_type=MESH)
    peers = [partner]
    peers += [at_y((y + d) % 4) for d in range(1, 4)]
    peers += [at_x((x + d) % 4) for d in range(1, 4)]
    peers += [at_z((z + d) % 8) for d in range(1, 8)]
    for peer in peers:
        pl.semaphore_signal(barrier, inc=1, device_id=peer, device_id_type=MESH)

    lanes = lax.broadcasted_iota(jnp.int32, (256, 256), 0)
    for k in range(12):
        pmat[k] = jnp.where(lanes == place_ref[k : k + 1, :], 1.0, 0.0).astype(BF16)
    omat[...] = jnp.where(
        lax.broadcasted_iota(jnp.int32, (C, C), 1) == order_ref[...], 1.0, 0.0
    ).astype(BF16)

    for copy in loads[:3]:
        copy.wait()
    for k in range(3):
        scol[0, k] = in4[k, :, 0, :]
        scol[1, k] = in4[k, :, T - 1, :]

    count = jnp.int32(len(peers))
    for d in around:
        count = count + there[d].astype(jnp.int32)
    pl.semaphore_wait(barrier, count)

    def halo(first, size, phase):
        copies = []
        for n, (dr, dc) in enumerate(around):
            span = pl.ds(first, size)
            if dc == 0:
                src = in4.at[span, 0 if dr < 0 else T - 1]
                dst = hrow.at[1 if dr < 0 else 0, span]
            elif dr == 0:
                src = scol.at[0 if dc < 0 else 1, span]
                dst = hcol.at[1 if dc < 0 else 0, span]
            else:
                src = scol.at[0 if dc < 0 else 1, span, pl.ds(0 if dr < 0 else 16, 16)]
                dst = hcor.at[(1 if dr < 0 else 0) * 2 + (1 if dc < 0 else 0), span]
            copies.append(
                (
                    (dr, dc),
                    pltpu.make_async_remote_copy(
                        src_ref=src, dst_ref=dst,
                        send_sem=hs_sem.at[phase, n], recv_sem=hr_sem.at[phase, n],
                        device_id=(row + dr, col + dc), device_id_type=MESH,
                    ),
                )
            )
        return copies

    def start(copies):
        for d, copy in copies:
            pl.when(there[d])(copy.start)

    def landed(copies):
        for d, copy in copies:
            pl.when(there[(-d[0], -d[1])])(copy.wait_recv)

    first = halo(0, 3, 0)
    start(first)

    @pl.when(row == 0)
    def _():
        hrow[0] = jnp.zeros((4, T, C), BF16)
        hcor[0] = jnp.zeros((4, 16, C), BF16)
        hcor[1] = jnp.zeros((4, 16, C), BF16)

    @pl.when(row == 15)
    def _():
        hrow[1] = jnp.zeros((4, T, C), BF16)
        hcor[2] = jnp.zeros((4, 16, C), BF16)
        hcor[3] = jnp.zeros((4, 16, C), BF16)

    @pl.when(jnp.logical_and(col == 0, row > 0))
    def _():
        hcor[0] = jnp.zeros((4, 16, C), BF16)

    @pl.when(jnp.logical_and(col == 0, row < 15))
    def _():
        hcor[2] = jnp.zeros((4, 16, C), BF16)

    @pl.when(col == 0)
    def _():
        hcol[0] = jnp.zeros((4, T, C), BF16)

    @pl.when(jnp.logical_and(col == 15, row > 0))
    def _():
        hcor[1] = jnp.zeros((4, 16, C), BF16)

    @pl.when(jnp.logical_and(col == 15, row < 15))
    def _():
        hcor[3] = jnp.zeros((4, 16, C), BF16)

    @pl.when(col == 15)
    def _():
        hcol[1] = jnp.zeros((4, T, C), BF16)

    loads[3].wait()
    for a in range(3):
        for b in range(3):
            wrem[0, a, :, (2 - b) * 64 : (3 - b) * 64] = wd[a * 3 + b, :, 256:320]
        wrem[0, a, :, 192:256] = jnp.zeros((C, 64), BF16)

    edge = lax.broadcasted_iota(jnp.int32, (T, C), 0)

    def shifted(k, act, with_rem):
        for side in range(2):
            hc32[side, 0:1, :] = hcor[side, k].astype(F32)[15:16]
            hc32[side, 1:33, :] = hcol[side, k].astype(F32)
            hc32[side, 33:34, :] = hcor[2 + side, k].astype(F32)[0:1]

        def emit(i, cells):
            left = hc32[0, pl.ds(i, 1), :]
            right = hc32[1, pl.ds(i, 1), :]
            now = cells.astype(F32)
            if act:
                now, left, right = silu(now), silu(left), silu(right)
            minus = jnp.where(edge == 0, left, pltpu.roll(now, 1, 0))
            plus = jnp.where(edge == T - 1, right, pltpu.roll(now, T - 1, 0))
            for s, v in enumerate((minus, now, plus)):
                v = v.astype(BF16)
                sh[s, i] = v
                if with_rem:
                    rem[i, :, s * 64 : (s + 1) * 64] = v[:, 256:320]
            if with_rem:
                rem[i, :, 192:256] = jnp.zeros((T, 64), BF16)

        emit(0, hrow[0, k])
        emit(T + 1, hrow[1, k])

        @pl.loop(0, T)
        def _(i):
            emit(i + 1, in4[k, i])

    def conv(w, wr, i0):
        total = jnp.zeros((512, C), F32)
        for a in range(3):
            rows = pl.ds(i0 + 2 - a, 16)
            for s in range(3):
                total += dot(sh[s, rows].reshape(512, C)[:, :256], w[a * 3 + 2 - s, :, :256], NT)
            total += dot(rem[rows].reshape(512, 256), wrem[wr, a], NT)
        return total

    def widened(dst):
        @pl.loop(0, 2)
        def _(h):
            for yy in range(4):
                lo, hi = (128, 320) if yy == 3 else (0, 256)
                total = jnp.zeros((544, 256), F32)
                for s in range(3):
                    cells = sh[s, pl.ds(h * 17, 17)].reshape(544, C)[:, lo:hi]
                    total += dot(cells, pmat[yy * 3 + s, : hi - lo])
                dst[yy, pl.ds(h * 544, 544), :] = total.astype(BF16)

    def turned(src):
        for n in range(4):
            gt[:, n * 256 : (n + 1) * 256] = dot(omat[...], src[n * 256 : (n + 1) * 256, :], NT).astype(BF16)

    def put(dst, yy, base, value):
        value = value.astype(BF16)
        for half in range(2):
            for q in range(2):
                for h in range(2):
                    dst[half, yy, h * 2 + q, pl.ds(base, 80), :] = value[
                        half * 160 + q * 80 : half * 160 + (q + 1) * 80, h * 128 : (h + 1) * 128
                    ]

    def weights(dst, src):
        @pl.loop(0, 3)
        def _(a):
            for yy in range(4):
                put(dst, yy, a * 80, dot(gt[...], src[yy, pl.ds(a * T, 1024), :]))

    landed(first)
    shifted(0, False, True)
    loads[4].wait()
    loads[5].wait()

    @pl.loop(0, 2)
    def _(h):
        grad = conv(wd, 0, h * 16)
        grad = (slope(pre[pl.ds(h * 16, 16)].reshape(512, C).astype(F32)) * grad).astype(BF16)
        dec[pl.ds(h * 512, 512), :] = grad
        in4[3, pl.ds(h * 16, 16)] = dot(grad, wz[...], NT).astype(BF16).reshape(16, T, C)

    scol[0, 3] = in4[3, :, 0, :]
    scol[1, 3] = in4[3, :, T - 1, :]
    second = halo(3, 1, 1)
    start(second)

    shifted(1, True, False)
    widened(xmid)
    turned(in4[3].reshape(1024, C))
    weights(ra, xmid)

    loads[6].wait()
    turned(dec)
    for yy in range(4):
        lo, hi = (128, 320) if yy == 3 else (0, 256)
        xout[...] = dot(cout[...].reshape(1024, C)[:, lo:hi], pmat[yy * 3, : hi - lo]).astype(BF16)
        put(ra, yy, 240, dot(gt[...], xout[...]))

    def pair(src, dst, n):
        return pltpu.make_async_remote_copy(
            src_ref=src, dst_ref=dst, send_sem=cs_sem.at[n], recv_sem=cr_sem.at[n],
            device_id=partner, device_id_type=MESH,
        )

    def remote(src, dst, n, peer):
        return pltpu.make_async_remote_copy(
            src_ref=src, dst_ref=dst, send_sem=ss_sem.at[n], recv_sem=sr_sem.at[n],
            device_id=peer, device_id_type=MESH,
        )

    class Stage:
        def __init__(self, base, pn, rows, split, zn, bufs, out, zt):
            self.base, self.pn, self.rows, self.split, self.zn = base, pn, rows, split, zn
            (self.r, self.c, self.y, self.x, self.e, self.f, self.y2, self.x2,
             self.d, self.zs, self.zr, self.fin, self.pin) = bufs
            self.out, self.zt = out, zt
            self.sent = []

        def go(self, copies):
            for copy in copies:
                copy.start()
            self.sent += copies
            return copies

        def one(self):
            self.k1 = self.go([pair(self.r.at[1 - core], self.c, self.pn)])

        def two(self):
            self.k1[0].wait_recv()

            @pl.loop(0, 4)
            def _(t):
                for u in range(4):
                    self.r[core, t, u] = (
                        self.r[core, t, u].astype(F32) + self.c[t, u].astype(F32)
                    ).astype(BF16)

            lo, hi = pl.ds(0, self.split), pl.ds(self.split, self.rows - self.split)
            self.k2 = []
            for d in (2, 1, 3):
                ty, tx = (y + d) % 4, (x + d) % 4
                self.k2.append(remote(self.r.at[core, ty, :, lo], self.y.at[d - 1], self.base + d - 1, at_y(ty)))
                self.k2.append(remote(self.r.at[core, :, tx, hi], self.x.at[d - 1], self.base + 2 + d, at_x(tx)))
            self.go(self.k2)

        def three(self):
            for copy in self.k2:
                copy.wait_recv()
            lo, hi = pl.ds(0, self.split), pl.ds(self.split, self.rows - self.split)

            @pl.loop(0, 4)
            def _(t):
                total = self.r[core, y, t, lo].astype(F32)
                for d in range(3):
                    total += self.y[d, t].astype(F32)
                self.e[t] = total.astype(BF16)
                total = self.r[core, t, x, hi].astype(F32)
                for d in range(3):
                    total += self.x[d, t].astype(F32)
                self.f[t] = total.astype(BF16)

            self.k3 = []
            for d in (2, 1, 3):
                ty, tx = (y + d) % 4, (x + d) % 4
                self.k3.append(remote(self.e.at[tx], self.x2.at[d - 1], self.base + 5 + d, at_x(tx)))
                self.k3.append(remote(self.f.at[ty], self.y2.at[d - 1], self.base + 8 + d, at_y(ty)))
            self.go(self.k3)

        def four(self):
            for copy in self.k3:
                copy.wait_recv()
            total = self.e[x].astype(F32)
            for d in range(3):
                total += self.x2[d].astype(F32)
            self.d[0 : self.split] = total.astype(BF16)
            total = self.f[y].astype(F32)
            for d in range(3):
                total += self.y2[d].astype(F32)
            self.d[self.split : self.rows] = total.astype(BF16)
            pick = jnp.where(
                lax.broadcasted_iota(jnp.int32, (8 * self.zn, self.rows), 1) == self.zt[...], 1.0, 0.0
            ).astype(BF16)
            self.zs[...] = dot(pick, self.d[...]).astype(BF16).reshape(8, self.zn, 128)
            self.k4 = []
            for d in (4, 3, 5, 2, 6, 1, 7):
                tz = (z + d) % 8
                self.k4.append(remote(self.zs.at[tz], self.zr.at[d - 1], self.base + 11 + d, at_z(tz)))
            self.go(self.k4)

        def five(self):
            for copy in self.k4:
                copy.wait_recv()
            total = self.zs[z].astype(F32)
            for d in range(7):
                total += self.zr[d].astype(F32)
            self.fin[...] = total
            self.out[core] = total
            self.k5 = self.go([pair(self.fin, self.pin, self.pn + 1)])

        def six(self):
            self.k5[0].wait_recv()
            self.out[1 - core] = self.pin[...]

    stage_a = Stage(0, 0, ROWS_A, SPLIT_A, ZA, (ra, ca, ya, xa, ea, fa, ya2, xa2, da, zsa, zra, fina, pina), out_a, za_ref)
    stage_b = Stage(19, 2, ROWS_B, SPLIT_B, ZB, (rb, cb, yb, xb, eb, fb, yb2, xb2, db, zsb, zrb, finb, pinb), out_b, zb_ref)

    stage_a.one()

    shifted(2, True, False)
    widened(xin)

    stage_a.two()

    loads[7].wait()
    for a in range(3):
        for b in range(3):
            wrem[1, a, :, (2 - b) * 64 : (3 - b) * 64] = wc[a * 3 + b, :, 256:320]
        wrem[1, a, :, 192:256] = jnp.zeros((C, 64), BF16)

    landed(second)
    shifted(3, False, True)

    @pl.loop(0, 2)
    def _(h):
        grad = conv(wc, 1, h * 16)
        grad = slope(in4[1, pl.ds(h * 16, 16)].reshape(512, C).astype(F32)) * grad
        mgrad[pl.ds(h * 512, 512), :] = grad.astype(BF16)

    turned(mgrad)
    weights(rb, xin)

    stage_b.one()
    stage_a.three()
    stage_b.two()
    stage_a.four()
    stage_b.three()
    stage_a.five()
    stage_b.four()
    stage_a.six()
    stage_b.five()
    stage_b.six()

    for copies in (first, second):
        for d, copy in copies:
            pl.when(there[d])(copy.wait_send)
    for copy in stage_a.sent + stage_b.sent:
        copy.wait_send()


def stage_buffers(rows, split, zn):
    rest = rows - split
    return [
        pltpu.VMEM((2, 4, 4, rows, 128), BF16),
        pltpu.VMEM((4, 4, rows, 128), BF16),
        pltpu.VMEM((3, 4, split, 128), BF16),
        pltpu.VMEM((3, 4, rest, 128), BF16),
        pltpu.VMEM((4, split, 128), BF16),
        pltpu.VMEM((4, rest, 128), BF16),
        pltpu.VMEM((3, rest, 128), BF16),
        pltpu.VMEM((3, split, 128), BF16),
        pltpu.VMEM((rows, 128), BF16),
        pltpu.VMEM((8, zn, 128), BF16),
        pltpu.VMEM((7, zn, 128), BF16),
        pltpu.VMEM((zn, 128), F32),
        pltpu.VMEM((zn, 128), F32),
    ]


def on_device(grad_out, dec_pre, ctrl_out, ctrl_mid, ctrl_in, dec_weight, zero_weight, ctrl_weight):
    tabs = [jnp.asarray(t) for t in tables()]
    anys = pl.BlockSpec(memory_space=pl.ANY)
    vmem = pl.BlockSpec(memory_space=pltpu.VMEM)
    out_a, out_b = pl.pallas_call(
        kernel,
        out_shape=(
            jax.ShapeDtypeStruct((2, ZA, 128), F32),
            jax.ShapeDtypeStruct((2, ZB, 128), F32),
        ),
        in_specs=[anys] * 8 + [vmem] * 4,
        out_specs=(vmem, vmem),
        scratch_shapes=[
            pltpu.VMEM((4, T, T, C), BF16),
            pltpu.VMEM((T, T, C), BF16),
            pltpu.VMEM((T, T, C), BF16),
            pltpu.VMEM((9, C, C), BF16),
            pltpu.VMEM((C, C), BF16),
            pltpu.VMEM((9, C, C), BF16),
            pltpu.VMEM((2, 4, T, C), BF16),
            pltpu.VMEM((2, 4, T, C), BF16),
            pltpu.VMEM((2, 4, T, C), BF16),
            pltpu.VMEM((4, 4, 16, C), BF16),
            pltpu.VMEM((2, 40, C), F32),
            pltpu.VMEM((3, T + 2, T, C), BF16),
            pltpu.VMEM((T + 2, T, 256), BF16),
            pltpu.VMEM((2, 3, C, 256), BF16),
            pltpu.VMEM((1024, C), BF16),
            pltpu.VMEM((4, 1088, 256), BF16),
            pltpu.VMEM((4, 1088, 256), BF16),
            pltpu.VMEM((1024, 256), BF16),
            pltpu.VMEM((12, 256, 256), BF16),
            pltpu.VMEM((C, C), BF16),
            pltpu.VMEM((C, 1024), BF16),
            pltpu.VMEM((1024, C), BF16),
        ]
        + stage_buffers(ROWS_A, SPLIT_A, ZA)
        + stage_buffers(ROWS_B, SPLIT_B, ZB)
        + [
            pltpu.SemaphoreType.DMA((8,)),
            pltpu.SemaphoreType.DMA((2, 8)),
            pltpu.SemaphoreType.DMA((2, 8)),
            pltpu.SemaphoreType.DMA((4,)),
            pltpu.SemaphoreType.DMA((4,)),
            pltpu.SemaphoreType.DMA((38,)),
            pltpu.SemaphoreType.DMA((38,)),
        ],
        compiler_params=pltpu.CompilerParams(
            collective_id=0, has_side_effects=True, vmem_limit_bytes=60 * 1024 * 1024
        ),
        name="fused",
    )(
        grad_out, dec_pre, ctrl_out, ctrl_mid, ctrl_in,
        dec_weight.reshape(9, C, C), zero_weight, ctrl_weight.reshape(9, C, C), *tabs,
    )
    core = lax.axis_index("row") % 2
    out_a = lax.dynamic_slice_in_dim(out_a, core * 64, 64, axis=2)
    out_b = lax.dynamic_slice_in_dim(out_b, core * 64, 64, axis=2)
    both = jnp.concatenate([out_a[:, :30, :60], out_b[:, :30, :60]], axis=1)
    both = both.reshape(2, 2, 3, 10, 3, 20).transpose(1, 2, 4, 5, 0, 3).reshape(2, 3, 3, 20, 20)
    grad_zero = out_a[:, 30:40, :20].transpose(2, 0, 1).reshape(20, 20)
    return (grad_zero, both[0], both[1])


def solution(mesh):
    tile = P("row", "col", None)
    return jax.shard_map(
        on_device,
        mesh=mesh,
        in_specs=(tile,) * 5 + (P(),) * 3,
        out_specs=(P("row", "col"), P(None, None, "row", "col"), P(None, None, "row", "col")),
        check_vma=False,
    )
```

```python
import jax
import jax.numpy as jnp
import numpy as np
from jax import lax
from jax.experimental import pallas as pl
from jax.experimental.pallas import tpu as pltpu
from jax.sharding import PartitionSpec as P

F32 = jnp.float32
BF16 = jnp.bfloat16
MESH = pl.DeviceIdType.MESH
NT = (((1,), (1,)), ((), ()))
NN = (((1,), (0,)), ((), ()))
C = 320
T = 32
ZA, ZB1, ZB2 = 48, 32, 16
N_SEM = 80


def dot(a, b, dims=NN):
    return lax.dot_general(a, b, dims, preferred_element_type=F32)


def silu(v):
    return v * jax.nn.sigmoid(v)


def slope(v):
    s = jax.nn.sigmoid(v)
    return s * (1.0 + v * (1.0 - s))


def tables():
    place = np.full((16, 256), -1, np.int32)
    for y in range(4):
        for s in range(3):
            for xh in range(2):
                for core in range(2):
                    for i in range(20):
                        lane = xh * 128 + core * 64 + s * 20 + i
                        c = y * 80 + xh * 40 + core * 20 + i
                        if c < 256:
                            place[y * 3 + s, lane] = c
                        else:
                            place[12, lane] = s * 64 + c - 256
    order = np.zeros((C, 1), np.int32)
    for core in range(2):
        for xl in range(2):
            for z in range(8):
                for i in range(10):
                    order[core * 160 + xl * 80 + z * 10 + i, 0] = (xl * 8 + z) * 20 + core * 10 + i
    deals = []
    for zn, groups in ((ZA, 4), (ZB1, 2), (ZB2, 1)):
        deal = np.full((8 * zn, 1), -1, np.int32)
        for z in range(8):
            for g in range(groups):
                for i in range(10):
                    deal[z * zn + g * 10 + i, 0] = g * 80 + z * 10 + i
        deals.append(deal)
    return place, order, *deals


def kernel(
    g_hbm, pre_hbm, cout_hbm, mid_hbm, cin_hbm, wd_hbm, wz_hbm, wc_hbm,
    place_hbm, order_hbm, deal_a_hbm, deal_b1_hbm, deal_b2_hbm,
    out_a, out_b1, out_b2,
    place_ref, order_ref, deal_a, deal_b1, deal_b2,
    in4, pre, cout, wd, wz, wc,
    scol, hrow, hcol, hcor, hc32,
    shg, remg, shm, remm, shi, remi,
    wrem, wn, tails, dec, pmat, omat, gt, mgrad,
    ra, rz, rb1, rb2,
    *rest,
):
    bufs, (load_sem, hs_sem, hr_sem, send_sem, recv_sem) = rest[:-5], rest[-5:]
    row = lax.axis_index("row")
    col = lax.axis_index("col")
    y, xh, core = row // 4, (row // 2) % 2, row % 2
    xl, z = col // 8, col % 8
    x = xh * 2 + xl

    def at_y(t):
        return ((t * 2 + xh) * 2 + core, col)

    def at_x(t):
        return ((y * 2 + t // 2) * 2 + core, (t % 2) * 8 + z)

    def at_z(t):
        return (row, xl * 8 + t)

    partner = (row + 1 - 2 * core, col)

    loads = [
        pltpu.make_async_copy(g_hbm, in4.at[0], load_sem.at[0]),
        pltpu.make_async_copy(mid_hbm, in4.at[1], load_sem.at[1]),
        pltpu.make_async_copy(cin_hbm, in4.at[2], load_sem.at[2]),
        pltpu.make_async_copy(wd_hbm, wd, load_sem.at[3]),
        pltpu.make_async_copy(pre_hbm, pre, load_sem.at[4]),
        pltpu.make_async_copy(wz_hbm, wz, load_sem.at[5]),
        pltpu.make_async_copy(wc_hbm, wc, load_sem.at[6]),
        pltpu.make_async_copy(cout_hbm, cout, load_sem.at[7]),
        pltpu.make_async_copy(order_hbm, order_ref, load_sem.at[8]),
        pltpu.make_async_copy(place_hbm, place_ref, load_sem.at[9]),
        pltpu.make_async_copy(deal_a_hbm, deal_a, load_sem.at[10]),
        pltpu.make_async_copy(deal_b1_hbm, deal_b1, load_sem.at[11]),
        pltpu.make_async_copy(deal_b2_hbm, deal_b2, load_sem.at[12]),
    ]
    for copy in loads:
        copy.start()

    has = {-1: (row > 0, col > 0), 1: (row < 15, col < 15), 0: (row >= 0, col >= 0)}
    around = [(dr, dc) for dr in (-1, 0, 1) for dc in (-1, 0, 1) if (dr, dc) != (0, 0)]
    there = {d: jnp.logical_and(has[d[0]][0], has[d[1]][1]) for d in around}

    barrier = pltpu.get_barrier_semaphore()
    for d in around:
        @pl.when(there[d])
        def _(d=d):
            pl.semaphore_signal(barrier, inc=1, device_id=(row + d[0], col + d[1]), device_id_type=MESH)
    peers = [partner]
    peers += [at_y((y + d) % 4) for d in range(1, 4)]
    peers += [at_x((x + d) % 4) for d in range(1, 4)]
    peers += [at_z((z + d) % 8) for d in range(1, 8)]
    for peer in peers:
        pl.semaphore_signal(barrier, inc=1, device_id=peer, device_id_type=MESH)

    def sides(n):
        scol[0, n] = in4[n, :, 0, :]
        scol[1, n] = in4[n, :, T - 1, :]

    loads[0].wait()
    sides(0)

    count = jnp.int32(len(peers))
    for d in around:
        count = count + there[d].astype(jnp.int32)
    pl.semaphore_wait(barrier, count)

    def halo(first, size, phase):
        copies = []
        for n, (dr, dc) in enumerate(around):
            span = pl.ds(first, size)
            if dc == 0:
                src = in4.at[span, 0 if dr < 0 else T - 1]
                dst = hrow.at[1 if dr < 0 else 0, span]
            elif dr == 0:
                src = scol.at[0 if dc < 0 else 1, span]
                dst = hcol.at[1 if dc < 0 else 0, span]
            else:
                src = scol.at[0 if dc < 0 else 1, span, pl.ds(0 if dr < 0 else 16, 16)]
                dst = hcor.at[(1 if dr < 0 else 0) * 2 + (1 if dc < 0 else 0), span]
            copies.append(
                (
                    (dr, dc),
                    pltpu.make_async_remote_copy(
                        src_ref=src, dst_ref=dst,
                        send_sem=hs_sem.at[phase, n], recv_sem=hr_sem.at[phase, n],
                        device_id=(row + dr, col + dc), device_id_type=MESH,
                    ),
                )
            )
        return copies

    def start(copies):
        for d, copy in copies:
            pl.when(there[d])(copy.start)

    def landed(copies):
        for d, copy in copies:
            pl.when(there[(-d[0], -d[1])])(copy.wait_recv)

    first = halo(0, 1, 0)
    start(first)
    loads[1].wait()
    loads[2].wait()
    sides(1)
    sides(2)
    acts = halo(1, 2, 1)
    start(acts)

    def clear(condition, ref, slot):
        @pl.when(condition)
        def _():
            ref[slot] = jnp.zeros(ref.shape[1:], BF16)

    clear(row == 0, hrow, 0)
    clear(row == 15, hrow, 1)
    clear(col == 0, hcol, 0)
    clear(col == 15, hcol, 1)
    for slot in range(4):
        edge_row = row == (0 if slot < 2 else 15)
        edge_col = col == (0 if slot % 2 == 0 else 15)
        clear(jnp.logical_or(edge_row, edge_col), hcor, slot)

    edge = lax.broadcasted_iota(jnp.int32, (T, C), 0)
    half_edge = lax.broadcasted_iota(jnp.int32, (16, C), 0)

    def columns(k, act):
        for side in range(2):
            parts = (hcor[side, k].astype(F32), hcol[side, k].astype(F32), hcor[2 + side, k].astype(F32))
            if act:
                parts = [silu(v) for v in parts]
            hc32[side, 0:1, :] = parts[0][15:16]
            hc32[side, 1:33, :] = parts[1]
            hc32[side, 33:34, :] = parts[2][0:1]

    def emit(sh, i, cells, act, sides):
        now = cells.astype(F32)
        if act:
            now = silu(now)
        minus, plus = pltpu.roll(now, 1, 0), pltpu.roll(now, T - 1, 0)
        if sides:
            minus = jnp.where(edge == 0, hc32[0, pl.ds(i, 1), :], minus)
            plus = jnp.where(edge == T - 1, hc32[1, pl.ds(i, 1), :], plus)
        sh[0, i] = minus.astype(BF16)
        sh[1, i] = now.astype(BF16)
        sh[2, i] = plus.astype(BF16)

    def inner(sh, k, act, sides):
        @pl.loop(0, T, unroll=4)
        def _(i):
            emit(sh, i + 1, in4[k, i], act, sides)

    def outer(sh, k, act):
        emit(sh, 0, hrow[0, k], act, True)
        emit(sh, T + 1, hrow[1, k], act, True)

    def patch(sh):
        @pl.loop(1, T + 1, unroll=4)
        def _(i):
            cells = sh[0, i, 0:16, :].astype(F32)
            sh[0, i, 0:16, :] = jnp.where(half_edge == 0, hc32[0, pl.ds(i, 1), :], cells).astype(BF16)
            cells = sh[2, i, 16:32, :].astype(F32)
            sh[2, i, 16:32, :] = jnp.where(half_edge == 15, hc32[1, pl.ds(i, 1), :], cells).astype(BF16)

    def gather_rem(sh, rem):
        @pl.loop(0, 2 * (T + 2) // 4)
        def _(n):
            span = pl.ds(n * 2, 2)
            for s in range(3):
                rem[span, :, s * 64 : (s + 1) * 64] = sh[s, span, :, 256:320]
            rem[span, :, 192:256] = jnp.zeros((2, T, 64), BF16)

    def arrange(w, slot):
        for a in range(3):
            for b in range(3):
                wrem[slot, a, :, (2 - b) * 64 : (3 - b) * 64] = w[a * 3 + b, :, 256:320]
                wn[slot, 2 - b, a * 64 : (a + 1) * 64, :] = w[a * 3 + b, 256:320, :256]
            wrem[slot, a, :, 192:256] = jnp.zeros((C, 64), BF16)
            wn[slot, 3, a * 64 : (a + 1) * 64, :] = wrem[slot, a, 256:320, :]
        wn[slot, :, 192:256, :] = jnp.zeros((4, 64, 256), BF16)

    def conv_tails(slot):
        @pl.loop(0, 2)
        def _(h):
            span = pl.ds(h * 17, 17)
            total = dot(remg[span].reshape(544, 256), wn[slot, 3], NT)
            for s in range(3):
                total += dot(shg[s, span].reshape(544, C)[:, :256], wn[slot, s], NT)
            tails[span] = total.reshape(17, T, 256)

    def conv(w, slot, i0):
        total = jnp.zeros((512, 256), F32)
        for a in range(3):
            span = pl.ds(i0 + 2 - a, 16)
            for s in range(3):
                total += dot(shg[s, span].reshape(512, C)[:, :256], w[a * 3 + 2 - s, :256, :256], NT)
            total += dot(remg[span].reshape(512, 256), wrem[slot, a, :256, :], NT)
        last = (
            tails[pl.ds(i0 + 2, 16)].reshape(512, 256)[:, :64]
            + tails[pl.ds(i0 + 1, 16)].reshape(512, 256)[:, 64:128]
            + tails[pl.ds(i0, 16)].reshape(512, 256)[:, 128:192]
        )
        return total, last

    def turned(src):
        for n in range(4):
            gt[:, n * 256 : (n + 1) * 256] = dot(omat[...], src[n * 256 : (n + 1) * 256, :], NT).astype(BF16)

    def halves(dst, base, lane, width, value):
        value = value.astype(BF16)
        for half in range(2):
            dst[half, base : base + 160, lane : lane + width] = value[half * 160 : (half + 1) * 160]

    def weights(dst, base, sh, rem, a):
        span = pl.ds(a, T)
        for s in range(3):
            halves(dst, base, s * 256, 256, dot(gt[...], sh[s, span].reshape(1024, C)[:, :256]))
        halves(dst, base, 768, 256, dot(gt[...], rem[span].reshape(1024, 256)))

    counter = [0]

    def remote(src, dst, peer):
        n = counter[0]
        counter[0] += 1
        return pltpu.make_async_remote_copy(
            src_ref=src, dst_ref=dst, send_sem=send_sem.at[n], recv_sem=recv_sem.at[n],
            device_id=peer, device_id_type=MESH,
        )

    class Stage:
        def __init__(self, out, deal, zn, sources, groups, rows, split, mine):
            self.out, self.deal, self.zn, self.sources, self.groups = out, deal, zn, sources, groups
            self.rows, self.split = rows, split
            self.landings = mine[: len(sources)]
            (self.d, self.ha, self.hb, self.pa, self.pb, self.e, self.f, self.ea, self.fb,
             self.j, self.zs, self.zr, self.fin, self.pin) = mine[len(sources):]
            self.sent = []

        def go(self, *copies):
            for copy in copies:
                copy.start()
            self.sent += copies
            return copies

        def one(self):
            self.k1 = self.go(*[
                remote(src.at[1 - core], dst, partner) for src, dst in zip(self.sources, self.landings)
            ])

        def put(self, base, yy, value):
            value = value.astype(BF16)
            for q in range(2):
                for h in range(2):
                    self.d[yy, h * 2 + q, pl.ds(base, 80), :] = value[
                        q * 80 : (q + 1) * 80, h * 128 : (h + 1) * 128
                    ]

        def two(self):
            for copy in self.k1:
                copy.wait_recv()

            def both(n, span, lanes):
                here = self.sources[n][core, span, lanes].astype(F32)
                return (here + self.landings[n][span, lanes].astype(F32)).astype(BF16)

            for g in range(self.groups):
                span = slice(g * 160, (g + 1) * 160)
                parts = [both(0, span, slice(s * 256, (s + 1) * 256)) for s in range(4)]
                for yy in range(4):
                    total = dot(parts[0], pmat[yy * 3])
                    for s in range(1, 3):
                        total += dot(parts[s], pmat[yy * 3 + s])
                    if yy == 3:
                        total += dot(parts[3], pmat[12])
                    self.put(g * 80, yy, total)
            if len(self.sources) > 1:
                main, last = (both(1, slice(0, 160), lanes) for lanes in (slice(0, 256), slice(256, 320)))
                for yy in range(4):
                    total = dot(main, pmat[yy * 3])
                    if yy == 3:
                        total += dot(last, pmat[12, 0:64])
                    self.put(self.groups * 80, yy, total)

            lo, hi = pl.ds(0, self.split), pl.ds(self.split, self.rows - self.split)
            far_y, far_x = (y + 2) % 4, (x + 2) % 4
            up_y, down_y, up_x, down_x = (y + 1) % 4, (y + 3) % 4, (x + 1) % 4, (x + 3) % 4
            low, high = pl.ds(0, 2), pl.ds(2, 2)
            self.k2 = self.go(
                remote(self.d.at[far_y, low, lo], self.ha.at[0], at_y(up_y)),
                remote(self.d.at[far_y, high, lo], self.ha.at[1], at_y(down_y)),
                remote(self.d.at[low, far_x, hi], self.hb.at[0], at_x(up_x)),
                remote(self.d.at[high, far_x, hi], self.hb.at[1], at_x(down_x)),
            )

        def relay(self):
            for copy in self.k2:
                copy.wait_recv()
            lo, hi = pl.ds(0, self.split), pl.ds(self.split, self.rows - self.split)
            for n in range(2):
                ty, tx = (y + 1 + 2 * n) % 4, (x + 1 + 2 * n) % 4
                for u in range(2):
                    t = 2 * n + u
                    self.d[ty, t, lo] = (self.d[ty, t, lo].astype(F32) + self.ha[n, u].astype(F32)).astype(BF16)
                    self.d[t, tx, hi] = (self.d[t, tx, hi].astype(F32) + self.hb[n, u].astype(F32)).astype(BF16)
            self.k3 = []
            for n in range(2):
                ty, tx = (y + 1 + 2 * n) % 4, (x + 1 + 2 * n) % 4
                self.k3 += self.go(
                    remote(self.d.at[ty, :, lo], self.pa.at[n], at_y(ty)),
                    remote(self.d.at[:, tx, hi], self.pb.at[n], at_x(tx)),
                )

        def three(self):
            for copy in self.k3:
                copy.wait_recv()
            lo, hi = pl.ds(0, self.split), pl.ds(self.split, self.rows - self.split)
            for t in range(4):
                total = self.d[y, t, lo].astype(F32) + self.pa[0, t].astype(F32) + self.pa[1, t].astype(F32)
                self.e[t] = total.astype(BF16)
                total = self.d[t, x, hi].astype(F32) + self.pb[0, t].astype(F32) + self.pb[1, t].astype(F32)
                self.f[t] = total.astype(BF16)
            self.k4 = []
            for d in (2, 1, 3):
                ty, tx = (y + d) % 4, (x + d) % 4
                self.k4 += self.go(
                    remote(self.e.at[tx], self.ea.at[d - 1], at_x(tx)),
                    remote(self.f.at[ty], self.fb.at[d - 1], at_y(ty)),
                )

        def four(self):
            for copy in self.k4:
                copy.wait_recv()
            total = self.e[x].astype(F32)
            for d in range(3):
                total += self.ea[d].astype(F32)
            self.j[0 : self.split] = total.astype(BF16)
            total = self.f[y].astype(F32)
            for d in range(3):
                total += self.fb[d].astype(F32)
            self.j[self.split : self.rows] = total.astype(BF16)
            pick = jnp.where(
                lax.broadcasted_iota(jnp.int32, (8 * self.zn, self.rows), 1) == self.deal[...], 1.0, 0.0
            ).astype(BF16)
            self.zs[...] = dot(pick, self.j[...]).astype(BF16).reshape(8, self.zn, 128)
            self.k5 = []
            for d in (4, 3, 5, 2, 6, 1, 7):
                tz = (z + d) % 8
                self.k5 += self.go(remote(self.zs.at[tz], self.zr.at[d - 1], at_z(tz)))

        def five(self):
            for copy in self.k5:
                copy.wait_recv()
            total = self.zs[z].astype(F32)
            for d in range(7):
                total += self.zr[d].astype(F32)
            self.fin[...] = total
            self.k6 = self.go(remote(self.fin, self.pin, partner))
            self.show(core, total)

        def show(self, side, value):
            self.out[side] = jnp.where(core == 0, value[:, :64], value[:, 64:])

        def six(self):
            self.k6[0].wait_recv()
            self.show(1 - core, self.pin[...])

    stage_a = Stage(out_a, deal_a, ZA, (ra, rz), 3, 320, 160, bufs[0:16])
    stage_b1 = Stage(out_b1, deal_b1, ZB1, (rb1,), 2, 160, 80, bufs[16:31])
    stage_b2 = Stage(out_b2, deal_b2, ZB2, (rb2,), 1, 80, 48, bufs[31:46])

    loads[3].wait()
    arrange(wd, 0)
    inner(shg, 0, False, False)
    landed(first)
    columns(0, False)
    outer(shg, 0, False)
    patch(shg)
    gather_rem(shg, remg)
    loads[4].wait()
    loads[5].wait()
    conv_tails(0)

    @pl.loop(0, 2)
    def _(h):
        main, last = conv(wd, 0, h * 16)
        rate = slope(pre[pl.ds(h * 16, 16)].reshape(512, C).astype(F32))
        dec[pl.ds(h * 512, 512), 0:256] = (rate[:, :256] * main).astype(BF16)
        dec[pl.ds(h * 512, 512), 256:320] = (rate[:, 256:] * last).astype(BF16)
        grad = dec[pl.ds(h * 512, 512), :]
        in4[3, pl.ds(h * 16, 16)] = dot(grad, wz[...], NT).astype(BF16).reshape(16, T, C)

    sides(3)
    second = halo(3, 1, 2)
    start(second)

    loads[8].wait()
    omat[...] = jnp.where(
        lax.broadcasted_iota(jnp.int32, (C, C), 1) == order_ref[...], 1.0, 0.0
    ).astype(BF16)
    landed(acts)
    columns(1, True)
    inner(shm, 1, True, True)
    outer(shm, 1, True)
    gather_rem(shm, remm)
    turned(in4[3].reshape(1024, C))
    for a in range(3):
        weights(ra, a * 160, shm, remm, a)
    loads[7].wait()
    turned(dec)
    halves(rz, 0, 0, C, dot(gt[...], cout[...].reshape(1024, C)))
    stage_a.one()
    for n in range(9, 13):
        loads[n].wait()
    depth = lax.broadcasted_iota(jnp.int32, (256, 256), 0)

    @pl.loop(0, 13)
    def _(k):
        pmat[k] = jnp.where(depth == place_ref[pl.ds(k, 1), :], 1.0, 0.0).astype(BF16)

    loads[6].wait()
    arrange(wc, 1)
    inner(shg, 3, False, False)
    landed(second)
    columns(3, False)
    outer(shg, 3, False)
    patch(shg)
    gather_rem(shg, remg)
    stage_a.two()
    columns(2, True)
    inner(shi, 2, True, True)
    outer(shi, 2, True)
    gather_rem(shi, remi)
    conv_tails(1)

    def second_half(h):
        main, last = conv(wc, 1, h * 16)
        rate = slope(in4[1, h * 16 : (h + 1) * 16].reshape(512, C).astype(F32))
        mgrad[h * 512 : (h + 1) * 512, 0:256] = (rate[:, :256] * main).astype(BF16)
        mgrad[h * 512 : (h + 1) * 512, 256:320] = (rate[:, 256:] * last).astype(BF16)

    second_half(0)
    stage_a.relay()
    second_half(1)
    turned(mgrad)
    for a in range(2):
        weights(rb1, a * 160, shi, remi, a)
    stage_b1.one()
    weights(rb2, 0, shi, remi, 2)
    stage_b2.one()
    stage_a.three()
    stage_b1.two()
    stage_b2.two()
    stage_a.four()
    stage_b1.relay()
    stage_b2.relay()
    stage_a.five()
    stage_b1.three()
    stage_b2.three()
    stage_a.six()
    stage_b1.four()
    stage_b2.four()
    stage_b1.five()
    stage_b2.five()
    stage_b1.six()
    stage_b2.six()

    for copies in (first, acts, second):
        for d, copy in copies:
            pl.when(there[d])(copy.wait_send)
    for copy in stage_a.sent + stage_b1.sent + stage_b2.sent:
        copy.wait_send()


def finish(a_ref, b1_ref, b2_ref, zero_ref, ctrl_ref, in_ref):
    def exact(a, b, dims):
        return lax.dot_general(a, b, dims, precision=lax.Precision.HIGHEST, preferred_element_type=F32)

    r = lax.broadcasted_iota(jnp.int32, (72, 64), 0)
    lane = lax.broadcasted_iota(jnp.int32, (72, 64), 1)
    sel = jnp.zeros((72, 64), F32)
    for s in range(3):
        inside = (r >= s * 24) & (r < s * 24 + 20)
        sel = jnp.where(inside & (lane - s * 20 == r - s * 24), 1.0, sel)
    for ref, groups, dst, base in ((a_ref, 4, ctrl_ref, 0), (b1_ref, 2, in_ref, 0), (b2_ref, 1, in_ref, 2)):
        zn = ref.shape[1]
        turn = exact(sel, ref[...].reshape(2 * zn, 64), NT)
        k = lax.broadcasted_iota(jnp.int32, (2 * zn, 20), 0)
        n = lax.broadcasted_iota(jnp.int32, (2 * zn, 20), 1)
        for g in range(groups):
            pick = jnp.where(k == jnp.where(n < 10, n, n - 10 + zn) + g * 10, 1.0, 0.0)
            value = exact(turn, pick, NN)
            if g == 3:
                zero_ref[...] = value[0:20]
            else:
                for s in range(3):
                    dst[(base + g) * 3 + s] = value[s * 24 : s * 24 + 20]


def stage_buffers(landings, rows, split, zn):
    rest = rows - split
    return [pltpu.VMEM(shape, BF16) for shape in landings] + [
        pltpu.VMEM((4, 4, rows, 128), BF16),
        pltpu.VMEM((2, 2, split, 128), BF16),
        pltpu.VMEM((2, 2, rest, 128), BF16),
        pltpu.VMEM((2, 4, split, 128), BF16),
        pltpu.VMEM((2, 4, rest, 128), BF16),
        pltpu.VMEM((4, split, 128), BF16),
        pltpu.VMEM((4, rest, 128), BF16),
        pltpu.VMEM((3, split, 128), BF16),
        pltpu.VMEM((3, rest, 128), BF16),
        pltpu.VMEM((rows, 128), BF16),
        pltpu.VMEM((8, zn, 128), BF16),
        pltpu.VMEM((7, zn, 128), BF16),
        pltpu.VMEM((zn, 128), F32),
        pltpu.VMEM((zn, 128), F32),
    ]


def on_device(grad_out, dec_pre, ctrl_out, ctrl_mid, ctrl_in, dec_weight, zero_weight, ctrl_weight):
    tabs = [jnp.asarray(t) for t in tables()]
    anys = pl.BlockSpec(memory_space=pl.ANY)
    vmem = pl.BlockSpec(memory_space=pltpu.VMEM)
    shifts = [pltpu.VMEM((3, T + 2, T, C), BF16), pltpu.VMEM((T + 2, T, 256), BF16)]
    blocks = pl.pallas_call(
        kernel,
        out_shape=[jax.ShapeDtypeStruct((2, zn, 64), F32) for zn in (ZA, ZB1, ZB2)],
        in_specs=[anys] * 13,
        out_specs=[vmem] * 3,
        scratch_shapes=[
            *[pltpu.VMEM(t.shape, jnp.int32) for t in tabs],
            pltpu.VMEM((4, T, T, C), BF16),
            pltpu.VMEM((T, T, C), BF16),
            pltpu.VMEM((T, T, C), BF16),
            pltpu.VMEM((9, C, C), BF16),
            pltpu.VMEM((C, C), BF16),
            pltpu.VMEM((9, C, C), BF16),
            pltpu.VMEM((2, 4, T, C), BF16),
            pltpu.VMEM((2, 4, T, C), BF16),
            pltpu.VMEM((2, 4, T, C), BF16),
            pltpu.VMEM((4, 4, 16, C), BF16),
            pltpu.VMEM((2, 40, C), F32),
            *shifts, *shifts, *shifts,
            pltpu.VMEM((2, 3, C, 256), BF16),
            pltpu.VMEM((2, 4, 256, 256), BF16),
            pltpu.VMEM((T + 2, T, 256), F32),
            pltpu.VMEM((1024, C), BF16),
            pltpu.VMEM((13, 256, 256), BF16),
            pltpu.VMEM((C, C), BF16),
            pltpu.VMEM((C, 1024), BF16),
            pltpu.VMEM((1024, C), BF16),
            pltpu.VMEM((2, 480, 1024), BF16),
            pltpu.VMEM((2, 160, C), BF16),
            pltpu.VMEM((2, 320, 1024), BF16),
            pltpu.VMEM((2, 160, 1024), BF16),
        ]
        + stage_buffers([(480, 1024), (160, C)], 320, 160, ZA)
        + stage_buffers([(320, 1024)], 160, 80, ZB1)
        + stage_buffers([(160, 1024)], 80, 48, ZB2)
        + [
            pltpu.SemaphoreType.DMA((13,)),
            pltpu.SemaphoreType.DMA((3, 8)),
            pltpu.SemaphoreType.DMA((3, 8)),
            pltpu.SemaphoreType.DMA((N_SEM,)),
            pltpu.SemaphoreType.DMA((N_SEM,)),
        ],
        compiler_params=pltpu.CompilerParams(
            collective_id=0, has_side_effects=True, vmem_limit_bytes=60 * 1024 * 1024
        ),
        name="fused",
    )(
        grad_out, dec_pre, ctrl_out, ctrl_mid, ctrl_in,
        dec_weight.reshape(9, C, C), zero_weight, ctrl_weight.reshape(9, C, C), *tabs,
    )

    grad_zero, grad_ctrl, grad_in = pl.pallas_call(
        finish,
        out_shape=[
            jax.ShapeDtypeStruct((20, 20), F32),
            jax.ShapeDtypeStruct((9, 20, 20), F32),
            jax.ShapeDtypeStruct((9, 20, 20), F32),
        ],
        in_specs=[vmem] * 3,
        out_specs=[vmem] * 3,
        name="finish",
    )(*blocks)
    return (grad_zero, grad_ctrl.reshape(3, 3, 20, 20), grad_in.reshape(3, 3, 20, 20))


def solution(mesh):
    tile = P("row", "col", None)
    return jax.shard_map(
        on_device,
        mesh=mesh,
        in_specs=(tile,) * 5 + (P(),) * 3,
        out_specs=(P("row", "col"), P(None, None, "row", "col"), P(None, None, "row", "col")),
        check_vma=False,
    )
```

```python
import jax
import jax.numpy as jnp
import numpy as np
from jax import lax
from jax.experimental import pallas as pl
from jax.experimental.pallas import tpu as pltpu
from jax.sharding import PartitionSpec as P

F32 = jnp.float32
BF16 = jnp.bfloat16
MESH = pl.DeviceIdType.MESH
NT = (((1,), (1,)), ((), ()))
NN = (((1,), (0,)), ((), ()))
C = 320
T = 32
ZN, ZC = 32, 16
N_SEM = 96


def dot(a, b, dims=NN):
    return lax.dot_general(a, b, dims, preferred_element_type=F32)


def silu(v):
    return v * jax.nn.sigmoid(v)


def slope(v):
    s = jax.nn.sigmoid(v)
    return s * (1.0 + v * (1.0 - s))


def tables():
    place = np.full((16, 256), -1, np.int32)
    for y in range(4):
        for s in range(3):
            for xh in range(2):
                for core in range(2):
                    for i in range(20):
                        lane = xh * 128 + core * 64 + s * 20 + i
                        c = y * 80 + xh * 40 + core * 20 + i
                        if c < 256:
                            place[y * 3 + s, lane] = c
                        else:
                            place[12, lane] = s * 64 + c - 256
    order = np.zeros((C, 1), np.int32)
    for core in range(2):
        for xl in range(2):
            for z in range(8):
                for i in range(10):
                    order[core * 160 + xl * 80 + z * 10 + i, 0] = (xl * 8 + z) * 20 + core * 10 + i
    deals = []
    for zn, groups in ((ZN, 3), (ZC, 1)):
        deal = np.full((8 * zn, 1), -1, np.int32)
        for z in range(8):
            for g in range(groups):
                for i in range(10):
                    deal[z * zn + g * 10 + i, 0] = g * 80 + z * 10 + i
        deals.append(deal)
    return place, order, *deals


def kernel(
    g_hbm, pre_hbm, cout_hbm, mid_hbm, cin_hbm, wd_hbm, wz_hbm, wc_hbm,
    place_hbm, order_hbm, deal_hbm, deal_c_hbm,
    out_a, out_b, out_c,
    place_ref, order_ref, deal, deal_c,
    in4, pre, cout, wd, wz, wc,
    scol, hrow, hcol, hcor, hc32,
    shg, remg, shm, remm, shi, remi,
    wrem, wn, tails, dec, pmat, omat, gt, mgrad,
    ra, rz, rb1, rb2,
    *rest,
):
    bufs, (load_sem, hs_sem, hr_sem, send_sem, recv_sem) = rest[:-5], rest[-5:]
    row = lax.axis_index("row")
    col = lax.axis_index("col")
    y, xh, core = row // 4, (row // 2) % 2, row % 2
    xl, z = col // 8, col % 8
    x = xh * 2 + xl

    def at_y(t):
        return ((t * 2 + xh) * 2 + core, col)

    def at_x(t):
        return ((y * 2 + t // 2) * 2 + core, (t % 2) * 8 + z)

    def at_z(t):
        return (row, xl * 8 + t)

    partner = (row + 1 - 2 * core, col)

    loads = [
        pltpu.make_async_copy(g_hbm, in4.at[0], load_sem.at[0]),
        pltpu.make_async_copy(mid_hbm, in4.at[1], load_sem.at[1]),
        pltpu.make_async_copy(cin_hbm, in4.at[2], load_sem.at[2]),
        pltpu.make_async_copy(wd_hbm, wd, load_sem.at[3]),
        pltpu.make_async_copy(pre_hbm, pre, load_sem.at[4]),
        pltpu.make_async_copy(wz_hbm, wz, load_sem.at[5]),
        pltpu.make_async_copy(wc_hbm, wc, load_sem.at[6]),
        pltpu.make_async_copy(cout_hbm, cout, load_sem.at[7]),
        pltpu.make_async_copy(order_hbm, order_ref, load_sem.at[8]),
        pltpu.make_async_copy(place_hbm, place_ref, load_sem.at[9]),
        pltpu.make_async_copy(deal_hbm, deal, load_sem.at[10]),
        pltpu.make_async_copy(deal_c_hbm, deal_c, load_sem.at[11]),
    ]
    loads[0].start()

    has = {-1: (row > 0, col > 0), 1: (row < 15, col < 15), 0: (row >= 0, col >= 0)}
    around = [(dr, dc) for dr in (-1, 0, 1) for dc in (-1, 0, 1) if (dr, dc) != (0, 0)]
    there = {d: jnp.logical_and(has[d[0]][0], has[d[1]][1]) for d in around}

    barrier = pltpu.get_barrier_semaphore()
    for d in around:
        @pl.when(there[d])
        def _(d=d):
            pl.semaphore_signal(barrier, inc=1, device_id=(row + d[0], col + d[1]), device_id_type=MESH)
    peers = [partner]
    peers += [at_y((y + d) % 4) for d in range(1, 4)]
    peers += [at_x((x + d) % 4) for d in range(1, 4)]
    peers += [at_z((z + d) % 8) for d in range(1, 8)]
    for peer in peers:
        pl.semaphore_signal(barrier, inc=1, device_id=peer, device_id_type=MESH)

    def sides(n):
        scol[0, n] = in4[n, :, 0, :]
        scol[1, n] = in4[n, :, T - 1, :]

    loads[0].wait()
    for copy in loads[1:]:
        copy.start()
    sides(0)

    count = jnp.int32(len(peers))
    for d in around:
        count = count + there[d].astype(jnp.int32)
    pl.semaphore_wait(barrier, count)

    def halo(first, size, phase):
        copies = []
        for n, (dr, dc) in enumerate(around):
            span = pl.ds(first, size)
            if dc == 0:
                src = in4.at[span, 0 if dr < 0 else T - 1]
                dst = hrow.at[1 if dr < 0 else 0, span]
            elif dr == 0:
                src = scol.at[0 if dc < 0 else 1, span]
                dst = hcol.at[1 if dc < 0 else 0, span]
            else:
                src = scol.at[0 if dc < 0 else 1, span, pl.ds(0 if dr < 0 else 16, 16)]
                dst = hcor.at[(1 if dr < 0 else 0) * 2 + (1 if dc < 0 else 0), span]
            copies.append(
                (
                    (dr, dc),
                    pltpu.make_async_remote_copy(
                        src_ref=src, dst_ref=dst,
                        send_sem=hs_sem.at[phase, n], recv_sem=hr_sem.at[phase, n],
                        device_id=(row + dr, col + dc), device_id_type=MESH,
                    ),
                )
            )
        return copies

    def start(copies):
        for d, copy in copies:
            pl.when(there[d])(copy.start)

    def landed(copies):
        for d, copy in copies:
            pl.when(there[(-d[0], -d[1])])(copy.wait_recv)

    first = halo(0, 1, 0)
    start(first)
    loads[1].wait()
    loads[2].wait()
    sides(1)
    sides(2)
    acts = halo(1, 2, 1)
    start(acts)

    def clear(condition, ref, slot):
        @pl.when(condition)
        def _():
            ref[slot] = jnp.zeros(ref.shape[1:], BF16)

    clear(row == 0, hrow, 0)
    clear(row == 15, hrow, 1)
    clear(col == 0, hcol, 0)
    clear(col == 15, hcol, 1)
    for slot in range(4):
        edge_row = row == (0 if slot < 2 else 15)
        edge_col = col == (0 if slot % 2 == 0 else 15)
        clear(jnp.logical_or(edge_row, edge_col), hcor, slot)

    edge = lax.broadcasted_iota(jnp.int32, (T, C), 0)
    half_edge = lax.broadcasted_iota(jnp.int32, (16, C), 0)

    def columns(k, act):
        for side in range(2):
            parts = (hcor[side, k].astype(F32), hcol[side, k].astype(F32), hcor[2 + side, k].astype(F32))
            if act:
                parts = [silu(v) for v in parts]
            hc32[side, 0:1, :] = parts[0][15:16]
            hc32[side, 1:33, :] = parts[1]
            hc32[side, 33:34, :] = parts[2][0:1]

    def emit(sh, i, cells, act, sides):
        now = cells.astype(F32)
        if act:
            now = silu(now)
        minus, plus = pltpu.roll(now, 1, 0), pltpu.roll(now, T - 1, 0)
        if sides:
            minus = jnp.where(edge == 0, hc32[0, pl.ds(i, 1), :], minus)
            plus = jnp.where(edge == T - 1, hc32[1, pl.ds(i, 1), :], plus)
        sh[0, i] = minus.astype(BF16)
        sh[1, i] = now.astype(BF16)
        sh[2, i] = plus.astype(BF16)

    def inner(sh, k, act, sides):
        @pl.loop(0, T, unroll=4)
        def _(i):
            emit(sh, i + 1, in4[k, i], act, sides)

    def outer(sh, k, act):
        emit(sh, 0, hrow[0, k], act, True)
        emit(sh, T + 1, hrow[1, k], act, True)

    def patch(sh):
        @pl.loop(1, T + 1, unroll=4)
        def _(i):
            cells = sh[0, i, 0:16, :].astype(F32)
            sh[0, i, 0:16, :] = jnp.where(half_edge == 0, hc32[0, pl.ds(i, 1), :], cells).astype(BF16)
            cells = sh[2, i, 16:32, :].astype(F32)
            sh[2, i, 16:32, :] = jnp.where(half_edge == 15, hc32[1, pl.ds(i, 1), :], cells).astype(BF16)

    def gather_rem(sh, rem):
        @pl.loop(0, 2 * (T + 2) // 4)
        def _(n):
            span = pl.ds(n * 2, 2)
            for s in range(3):
                rem[span, :, s * 64 : (s + 1) * 64] = sh[s, span, :, 256:320]
            rem[span, :, 192:256] = jnp.zeros((2, T, 64), BF16)

    def arrange(w, slot):
        for a in range(3):
            for b in range(3):
                wrem[slot, a, :, (2 - b) * 64 : (3 - b) * 64] = w[a * 3 + b, :, 256:320]
                wn[slot, 2 - b, a * 64 : (a + 1) * 64, :] = w[a * 3 + b, 256:320, :256]
            wrem[slot, a, :, 192:256] = jnp.zeros((C, 64), BF16)
            wn[slot, 3, a * 64 : (a + 1) * 64, :] = wrem[slot, a, 256:320, :]
        wn[slot, :, 192:256, :] = jnp.zeros((4, 64, 256), BF16)

    def conv_tails(slot):
        @pl.loop(0, 2)
        def _(h):
            span = pl.ds(h * 17, 17)
            total = dot(remg[span].reshape(544, 256), wn[slot, 3], NT)
            for s in range(3):
                total += dot(shg[s, span].reshape(544, C)[:, :256], wn[slot, s], NT)
            tails[span] = total.reshape(17, T, 256)

    def conv(w, slot, i0):
        total = jnp.zeros((512, 256), F32)
        for a in range(3):
            span = pl.ds(i0 + 2 - a, 16)
            for s in range(3):
                total += dot(shg[s, span].reshape(512, C)[:, :256], w[a * 3 + 2 - s, :256, :256], NT)
            total += dot(remg[span].reshape(512, 256), wrem[slot, a, :256, :], NT)
        last = (
            tails[pl.ds(i0 + 2, 16)].reshape(512, 256)[:, :64]
            + tails[pl.ds(i0 + 1, 16)].reshape(512, 256)[:, 64:128]
            + tails[pl.ds(i0, 16)].reshape(512, 256)[:, 128:192]
        )
        return total, last

    def turned(src):
        for n in range(4):
            gt[:, n * 256 : (n + 1) * 256] = dot(omat[...], src[n * 256 : (n + 1) * 256, :], NT).astype(BF16)

    def halves(dst, base, lane, width, value):
        value = value.astype(BF16)
        for half in range(2):
            dst[half, base : base + 160, lane : lane + width] = value[half * 160 : (half + 1) * 160]

    def weights(dst, base, sh, rem, a):
        span = pl.ds(a, T)
        for s in range(3):
            halves(dst, base, s * 256, 256, dot(gt[...], sh[s, span].reshape(1024, C)[:, :256]))
        halves(dst, base, 768, 256, dot(gt[...], rem[span].reshape(1024, 256)))

    counter = [0]

    def remote(src, dst, peer):
        n = counter[0]
        counter[0] += 1
        return pltpu.make_async_remote_copy(
            src_ref=src, dst_ref=dst, send_sem=send_sem.at[n], recv_sem=recv_sem.at[n],
            device_id=peer, device_id_type=MESH,
        )

    class Stage:
        def __init__(self, source, groups, rows, split, mine):
            self.source, self.groups, self.rows, self.split = source, groups, rows, split
            (self.landing, self.d, self.ha, self.hb, self.pa, self.pb,
             self.e, self.f, self.ea, self.fb) = mine
            self.sent = []

        def go(self, *copies):
            for copy in copies:
                copy.start()
            self.sent += copies
            return copies

        def one(self):
            self.k1 = self.go(remote(self.source.at[1 - core], self.landing, partner))

        def put(self, base, yy, value):
            value = value.astype(BF16)
            for q in range(2):
                for h in range(2):
                    self.d[yy, h * 2 + q, pl.ds(base, 80), :] = value[
                        q * 80 : (q + 1) * 80, h * 128 : (h + 1) * 128
                    ]

        def two(self):
            for copy in self.k1:
                copy.wait_recv()

            def both(span, lanes):
                here = self.source[core, span, lanes].astype(F32)
                return (here + self.landing[span, lanes].astype(F32)).astype(BF16)

            for g in range(self.groups):
                span = slice(g * 160, (g + 1) * 160)
                parts = [both(span, slice(s * 256, (s + 1) * 256)) for s in range(4)]
                for yy in range(4):
                    total = dot(parts[0], pmat[yy * 3])
                    for s in range(1, 3):
                        total += dot(parts[s], pmat[yy * 3 + s])
                    if yy == 3:
                        total += dot(parts[3], pmat[12])
                    self.put(g * 80, yy, total)
            if self.groups == 0:
                main, last = (both(slice(0, 160), lanes) for lanes in (slice(0, 256), slice(256, 320)))
                for yy in range(4):
                    total = dot(main, pmat[yy * 3])
                    if yy == 3:
                        total += dot(last, pmat[12, 0:64])
                    self.put(0, yy, total)

            lo, hi = pl.ds(0, self.split), pl.ds(self.split, self.rows - self.split)
            far_y, far_x = (y + 2) % 4, (x + 2) % 4
            up_y, down_y, up_x, down_x = (y + 1) % 4, (y + 3) % 4, (x + 1) % 4, (x + 3) % 4
            low, high = pl.ds(0, 2), pl.ds(2, 2)
            self.k2 = self.go(
                remote(self.d.at[far_y, low, lo], self.ha.at[0], at_y(up_y)),
                remote(self.d.at[far_y, high, lo], self.ha.at[1], at_y(down_y)),
                remote(self.d.at[low, far_x, hi], self.hb.at[0], at_x(up_x)),
                remote(self.d.at[high, far_x, hi], self.hb.at[1], at_x(down_x)),
            )

        def relay(self):
            for copy in self.k2:
                copy.wait_recv()
            lo, hi = pl.ds(0, self.split), pl.ds(self.split, self.rows - self.split)
            for n in range(2):
                ty, tx = (y + 1 + 2 * n) % 4, (x + 1 + 2 * n) % 4
                for u in range(2):
                    t = 2 * n + u
                    self.d[ty, t, lo] = (self.d[ty, t, lo].astype(F32) + self.ha[n, u].astype(F32)).astype(BF16)
                    self.d[t, tx, hi] = (self.d[t, tx, hi].astype(F32) + self.hb[n, u].astype(F32)).astype(BF16)
            self.k3 = []
            for n in range(2):
                ty, tx = (y + 1 + 2 * n) % 4, (x + 1 + 2 * n) % 4
                self.k3 += self.go(
                    remote(self.d.at[ty, :, lo], self.pa.at[n], at_y(ty)),
                    remote(self.d.at[:, tx, hi], self.pb.at[n], at_x(tx)),
                )

        def three(self):
            for copy in self.k3:
                copy.wait_recv()
            lo, hi = pl.ds(0, self.split), pl.ds(self.split, self.rows - self.split)
            for t in range(4):
                total = self.d[y, t, lo].astype(F32) + self.pa[0, t].astype(F32) + self.pa[1, t].astype(F32)
                self.e[t] = total.astype(BF16)
                total = self.d[t, x, hi].astype(F32) + self.pb[0, t].astype(F32) + self.pb[1, t].astype(F32)
                self.f[t] = total.astype(BF16)
            self.k4 = []
            for d in (2, 1, 3):
                ty, tx = (y + d) % 4, (x + d) % 4
                self.k4 += self.go(
                    remote(self.e.at[tx], self.ea.at[d - 1], at_x(tx)),
                    remote(self.f.at[ty], self.fb.at[d - 1], at_y(ty)),
                )

        def collect(self, j, base):
            for copy in self.k4:
                copy.wait_recv()
            total = self.e[x].astype(F32)
            for d in range(3):
                total += self.ea[d].astype(F32)
            j[base : base + self.split] = total.astype(BF16)
            total = self.f[y].astype(F32)
            for d in range(3):
                total += self.fb[d].astype(F32)
            j[base + self.split : base + self.rows] = total.astype(BF16)

    class Last(Stage):
        def __init__(self, out, table, zn, rows, parts, mine):
            self.out, self.table, self.zn, self.rows, self.parts = out, table, zn, rows, parts
            self.j, self.zs, self.zr, self.fin, self.pin = mine
            self.sent = []

        def four(self):
            base = 0
            for part in self.parts:
                part.collect(self.j, base)
                base += part.rows
            pick = jnp.where(
                lax.broadcasted_iota(jnp.int32, (8 * self.zn, self.rows), 1) == self.table[...], 1.0, 0.0
            ).astype(BF16)
            self.zs[...] = dot(pick, self.j[...]).astype(BF16).reshape(8, self.zn, 128)
            self.k5 = []
            for d in (4, 3, 5, 2, 6, 1, 7):
                tz = (z + d) % 8
                self.k5 += self.go(remote(self.zs.at[tz], self.zr.at[d - 1], at_z(tz)))

        def five(self):
            for copy in self.k5:
                copy.wait_recv()
            total = self.zs[z].astype(F32)
            for d in range(7):
                total += self.zr[d].astype(F32)
            self.fin[...] = total
            self.k6 = self.go(remote(self.fin, self.pin, partner))
            self.show(core, total)

        def show(self, side, value):
            self.out[side] = jnp.where(core == 0, value[:, :64], value[:, 64:])

        def six(self):
            self.k6[0].wait_recv()
            self.show(1 - core, self.pin[...])

    stage_a = Stage(ra, 3, 240, 128, bufs[0:10])
    stage_b1 = Stage(rb1, 2, 160, 80, bufs[10:20])
    stage_b2 = Stage(rb2, 1, 80, 48, bufs[20:30])
    stage_c = Stage(rz, 0, 80, 48, bufs[30:40])
    last_a = Last(out_a, deal, ZN, 240, (stage_a,), bufs[40:45])
    last_b = Last(out_b, deal, ZN, 240, (stage_b1, stage_b2), bufs[45:50])
    last_c = Last(out_c, deal_c, ZC, 80, (stage_c,), bufs[50:55])

    loads[3].wait()
    arrange(wd, 0)
    inner(shg, 0, False, False)
    landed(first)
    columns(0, False)
    outer(shg, 0, False)
    patch(shg)
    gather_rem(shg, remg)
    loads[4].wait()
    loads[5].wait()
    conv_tails(0)

    @pl.loop(0, 2)
    def _(h):
        main, last = conv(wd, 0, h * 16)
        rate = slope(pre[pl.ds(h * 16, 16)].reshape(512, C).astype(F32))
        dec[pl.ds(h * 512, 512), 0:256] = (rate[:, :256] * main).astype(BF16)
        dec[pl.ds(h * 512, 512), 256:320] = (rate[:, 256:] * last).astype(BF16)
        grad = dec[pl.ds(h * 512, 512), :]
        in4[3, pl.ds(h * 16, 16)] = dot(grad, wz[...], NT).astype(BF16).reshape(16, T, C)

    sides(3)
    second = halo(3, 1, 2)
    start(second)

    loads[8].wait()
    omat[...] = jnp.where(
        lax.broadcasted_iota(jnp.int32, (C, C), 1) == order_ref[...], 1.0, 0.0
    ).astype(BF16)
    landed(acts)
    columns(1, True)
    inner(shm, 1, True, True)
    outer(shm, 1, True)
    gather_rem(shm, remm)
    turned(in4[3].reshape(1024, C))
    for a in range(3):
        weights(ra, a * 160, shm, remm, a)
    stage_a.one()
    for n in range(9, 12):
        loads[n].wait()
    depth = lax.broadcasted_iota(jnp.int32, (256, 256), 0)

    @pl.loop(0, 13)
    def _(k):
        pmat[k] = jnp.where(depth == place_ref[pl.ds(k, 1), :], 1.0, 0.0).astype(BF16)

    loads[6].wait()
    arrange(wc, 1)
    inner(shg, 3, False, False)
    landed(second)
    columns(3, False)
    outer(shg, 3, False)
    patch(shg)
    gather_rem(shg, remg)
    stage_a.two()
    columns(2, True)
    inner(shi, 2, True, True)
    outer(shi, 2, True)
    gather_rem(shi, remi)
    conv_tails(1)

    def second_half(h):
        main, last = conv(wc, 1, h * 16)
        rate = slope(in4[1, h * 16 : (h + 1) * 16].reshape(512, C).astype(F32))
        mgrad[h * 512 : (h + 1) * 512, 0:256] = (rate[:, :256] * main).astype(BF16)
        mgrad[h * 512 : (h + 1) * 512, 256:320] = (rate[:, 256:] * last).astype(BF16)

    second_half(0)
    stage_a.relay()
    second_half(1)
    turned(mgrad)
    for a in range(2):
        weights(rb1, a * 160, shi, remi, a)
    stage_b1.one()
    weights(rb2, 0, shi, remi, 2)
    stage_b2.one()
    stage_a.three()
    stage_b1.two()
    stage_b2.two()
    loads[7].wait()
    turned(dec)
    halves(rz, 0, 0, C, dot(gt[...], cout[...].reshape(1024, C)))
    stage_c.one()
    stage_b1.relay()
    stage_b2.relay()
    last_a.four()
    stage_c.two()
    stage_b1.three()
    stage_b2.three()
    stage_c.relay()
    last_a.five()
    last_b.four()
    stage_c.three()
    last_a.six()
    last_c.four()
    last_b.five()
    last_b.six()
    last_c.five()
    last_c.six()

    for copies in (first, acts, second):
        for d, copy in copies:
            pl.when(there[d])(copy.wait_send)
    for part in (stage_a, stage_b1, stage_b2, stage_c, last_a, last_b, last_c):
        for copy in part.sent:
            copy.wait_send()


def finish(a_ref, b_ref, c_ref, zero_ref, ctrl_ref, in_ref):
    def exact(a, b, dims):
        return lax.dot_general(a, b, dims, precision=lax.Precision.HIGHEST, preferred_element_type=F32)

    r = lax.broadcasted_iota(jnp.int32, (72, 64), 0)
    lane = lax.broadcasted_iota(jnp.int32, (72, 64), 1)
    sel = jnp.zeros((72, 64), F32)
    for s in range(3):
        inside = (r >= s * 24) & (r < s * 24 + 20)
        sel = jnp.where(inside & (lane - s * 20 == r - s * 24), 1.0, sel)
    for ref, groups, dst in ((a_ref, 3, ctrl_ref), (b_ref, 3, in_ref), (c_ref, 1, None)):
        zn = ref.shape[1]
        turn = exact(sel, ref[...].reshape(2 * zn, 64), NT)
        k = lax.broadcasted_iota(jnp.int32, (2 * zn, 20), 0)
        n = lax.broadcasted_iota(jnp.int32, (2 * zn, 20), 1)
        for g in range(groups):
            pick = jnp.where(k == jnp.where(n < 10, n, n - 10 + zn) + g * 10, 1.0, 0.0)
            value = exact(turn, pick, NN)
            if dst is None:
                zero_ref[...] = value[0:20]
            else:
                for s in range(3):
                    dst[g * 3 + s] = value[s * 24 : s * 24 + 20]


def stage_buffers(landing, rows, split):
    rest = rows - split
    return [
        pltpu.VMEM(landing, BF16),
        pltpu.VMEM((4, 4, rows, 128), BF16),
        pltpu.VMEM((2, 2, split, 128), BF16),
        pltpu.VMEM((2, 2, rest, 128), BF16),
        pltpu.VMEM((2, 4, split, 128), BF16),
        pltpu.VMEM((2, 4, rest, 128), BF16),
        pltpu.VMEM((4, split, 128), BF16),
        pltpu.VMEM((4, rest, 128), BF16),
        pltpu.VMEM((3, split, 128), BF16),
        pltpu.VMEM((3, rest, 128), BF16),
    ]


def last_buffers(rows, zn):
    return [
        pltpu.VMEM((rows, 128), BF16),
        pltpu.VMEM((8, zn, 128), BF16),
        pltpu.VMEM((7, zn, 128), BF16),
        pltpu.VMEM((zn, 128), F32),
        pltpu.VMEM((zn, 128), F32),
    ]


def on_device(grad_out, dec_pre, ctrl_out, ctrl_mid, ctrl_in, dec_weight, zero_weight, ctrl_weight):
    tabs = [jnp.asarray(t) for t in tables()]
    anys = pl.BlockSpec(memory_space=pl.ANY)
    vmem = pl.BlockSpec(memory_space=pltpu.VMEM)
    shifts = [pltpu.VMEM((3, T + 2, T, C), BF16), pltpu.VMEM((T + 2, T, 256), BF16)]
    blocks = pl.pallas_call(
        kernel,
        out_shape=[jax.ShapeDtypeStruct((2, zn, 64), F32) for zn in (ZN, ZN, ZC)],
        in_specs=[anys] * 12,
        out_specs=[vmem] * 3,
        scratch_shapes=[
            *[pltpu.VMEM(t.shape, jnp.int32) for t in tabs],
            pltpu.VMEM((4, T, T, C), BF16),
            pltpu.VMEM((T, T, C), BF16),
            pltpu.VMEM((T, T, C), BF16),
            pltpu.VMEM((9, C, C), BF16),
            pltpu.VMEM((C, C), BF16),
            pltpu.VMEM((9, C, C), BF16),
            pltpu.VMEM((2, 4, T, C), BF16),
            pltpu.VMEM((2, 4, T, C), BF16),
            pltpu.VMEM((2, 4, T, C), BF16),
            pltpu.VMEM((4, 4, 16, C), BF16),
            pltpu.VMEM((2, 40, C), F32),
            *shifts, *shifts, *shifts,
            pltpu.VMEM((2, 3, C, 256), BF16),
            pltpu.VMEM((2, 4, 256, 256), BF16),
            pltpu.VMEM((T + 2, T, 256), F32),
            pltpu.VMEM((1024, C), BF16),
            pltpu.VMEM((13, 256, 256), BF16),
            pltpu.VMEM((C, C), BF16),
            pltpu.VMEM((C, 1024), BF16),
            pltpu.VMEM((1024, C), BF16),
            pltpu.VMEM((2, 480, 1024), BF16),
            pltpu.VMEM((2, 160, C), BF16),
            pltpu.VMEM((2, 320, 1024), BF16),
            pltpu.VMEM((2, 160, 1024), BF16),
        ]
        + stage_buffers((480, 1024), 240, 128)
        + stage_buffers((320, 1024), 160, 80)
        + stage_buffers((160, 1024), 80, 48)
        + stage_buffers((160, C), 80, 48)
        + last_buffers(240, ZN)
        + last_buffers(240, ZN)
        + last_buffers(80, ZC)
        + [
            pltpu.SemaphoreType.DMA((12,)),
            pltpu.SemaphoreType.DMA((3, 8)),
            pltpu.SemaphoreType.DMA((3, 8)),
            pltpu.SemaphoreType.DMA((N_SEM,)),
            pltpu.SemaphoreType.DMA((N_SEM,)),
        ],
        compiler_params=pltpu.CompilerParams(
            collective_id=0, has_side_effects=True, vmem_limit_bytes=60 * 1024 * 1024
        ),
        name="fused",
    )(
        grad_out, dec_pre, ctrl_out, ctrl_mid, ctrl_in,
        dec_weight.reshape(9, C, C), zero_weight, ctrl_weight.reshape(9, C, C), *tabs,
    )

    grad_zero, grad_ctrl, grad_in = pl.pallas_call(
        finish,
        out_shape=[
            jax.ShapeDtypeStruct((20, 20), F32),
            jax.ShapeDtypeStruct((9, 20, 20), F32),
            jax.ShapeDtypeStruct((9, 20, 20), F32),
        ],
        in_specs=[vmem] * 3,
        out_specs=[vmem] * 3,
        name="finish",
    )(*blocks)
    return (grad_zero, grad_ctrl.reshape(3, 3, 20, 20), grad_in.reshape(3, 3, 20, 20))


def solution(mesh):
    tile = P("row", "col", None)
    return jax.shard_map(
        on_device,
        mesh=mesh,
        in_specs=(tile,) * 5 + (P(),) * 3,
        out_specs=(P("row", "col"), P(None, None, "row", "col"), P(None, None, "row", "col")),
        check_vma=False,
    )
```

```python
import jax
import jax.numpy as jnp
import numpy as np
from jax import lax
from jax.experimental import pallas as pl
from jax.experimental.pallas import tpu as pltpu
from jax.sharding import PartitionSpec as P

F32 = jnp.float32
BF16 = jnp.bfloat16
MESH = pl.DeviceIdType.MESH
NT = (((1,), (1,)), ((), ()))
NN = (((1,), (0,)), ((), ()))
C = 320
T = 32
ZN, ZC = 32, 16
N_SEM = 96


def dot(a, b, dims=NN):
    return lax.dot_general(a, b, dims, preferred_element_type=F32)


def silu(v):
    return v * jax.nn.sigmoid(v)


def slope(v):
    s = jax.nn.sigmoid(v)
    return s * (1.0 + v * (1.0 - s))


def tables():
    place = np.full((16, 256), -1, np.int32)
    for y in range(4):
        for s in range(3):
            for xh in range(2):
                for core in range(2):
                    for i in range(20):
                        lane = xh * 128 + core * 64 + s * 20 + i
                        c = y * 80 + xh * 40 + core * 20 + i
                        if c < 256:
                            place[y * 3 + s, lane] = c
                        else:
                            place[12, lane] = s * 64 + c - 256
    order = np.zeros((C, 1), np.int32)
    for core in range(2):
        for xl in range(2):
            for z in range(8):
                for i in range(10):
                    order[core * 160 + xl * 80 + z * 10 + i, 0] = (xl * 8 + z) * 20 + core * 10 + i
    deals = []
    for zn, groups in ((ZN, 3), (ZC, 1)):
        deal = np.full((8 * zn, 1), -1, np.int32)
        for z in range(8):
            for g in range(groups):
                for i in range(10):
                    deal[z * zn + g * 10 + i, 0] = g * 80 + z * 10 + i
        deals.append(deal)
    return place, order, *deals


def kernel(
    g_hbm, pre_hbm, cout_hbm, mid_hbm, cin_hbm, wd_hbm, wz_hbm, wc_hbm,
    place_hbm, order_hbm, deal_hbm, deal_c_hbm,
    out_a, out_b, out_c,
    place_ref, order_ref, deal, deal_c,
    in4, pre, cout, wd, wz, wc,
    scol, hrow, hcol, hcor, hc32,
    shg, remg, shm, remm, shi, remi,
    wrem, wn, tails, acc, rate1, rate2, dec, pmat, omat, gt, mgrad,
    ra, rz, rb1, rb2,
    *rest,
):
    bufs, (load_sem, hs_sem, hr_sem, send_sem, recv_sem) = rest[:-5], rest[-5:]
    row = lax.axis_index("row")
    col = lax.axis_index("col")
    y, xh, core = row // 4, (row // 2) % 2, row % 2
    xl, z = col // 8, col % 8
    x = xh * 2 + xl

    def at_y(t):
        return ((t * 2 + xh) * 2 + core, col)

    def at_x(t):
        return ((y * 2 + t // 2) * 2 + core, (t % 2) * 8 + z)

    def at_z(t):
        return (row, xl * 8 + t)

    partner = (row + 1 - 2 * core, col)

    loads = [
        pltpu.make_async_copy(g_hbm, in4.at[0], load_sem.at[0]),
        pltpu.make_async_copy(mid_hbm, in4.at[1], load_sem.at[1]),
        pltpu.make_async_copy(cin_hbm, in4.at[2], load_sem.at[2]),
        pltpu.make_async_copy(wd_hbm, wd, load_sem.at[3]),
        pltpu.make_async_copy(pre_hbm, pre, load_sem.at[4]),
        pltpu.make_async_copy(wz_hbm, wz, load_sem.at[5]),
        pltpu.make_async_copy(wc_hbm, wc, load_sem.at[6]),
        pltpu.make_async_copy(cout_hbm, cout, load_sem.at[7]),
        pltpu.make_async_copy(order_hbm, order_ref, load_sem.at[8]),
        pltpu.make_async_copy(place_hbm, place_ref, load_sem.at[9]),
        pltpu.make_async_copy(deal_hbm, deal, load_sem.at[10]),
        pltpu.make_async_copy(deal_c_hbm, deal_c, load_sem.at[11]),
    ]
    loads[0].start()

    has = {-1: (row > 0, col > 0), 1: (row < 15, col < 15), 0: (row >= 0, col >= 0)}
    around = [(dr, dc) for dr in (-1, 0, 1) for dc in (-1, 0, 1) if (dr, dc) != (0, 0)]
    there = {d: jnp.logical_and(has[d[0]][0], has[d[1]][1]) for d in around}

    barrier = pltpu.get_barrier_semaphore()
    for d in around:
        @pl.when(there[d])
        def _(d=d):
            pl.semaphore_signal(barrier, inc=1, device_id=(row + d[0], col + d[1]), device_id_type=MESH)
    peers = [partner]
    peers += [at_y((y + d) % 4) for d in range(1, 4)]
    peers += [at_x((x + d) % 4) for d in range(1, 4)]
    peers += [at_z((z + d) % 8) for d in range(1, 8)]
    for peer in peers:
        pl.semaphore_signal(barrier, inc=1, device_id=peer, device_id_type=MESH)

    edge = lax.broadcasted_iota(jnp.int32, (T, C), 0)
    half_edge = lax.broadcasted_iota(jnp.int32, (16, C), 0)

    def columns(k, act):
        for side in range(2):
            parts = (hcor[side, k].astype(F32), hcol[side, k].astype(F32), hcor[2 + side, k].astype(F32))
            if act:
                parts = [silu(v) for v in parts]
            hc32[side, 0:1, :] = parts[0][15:16]
            hc32[side, 1:33, :] = parts[1]
            hc32[side, 33:34, :] = parts[2][0:1]

    def emit(sh, i, cells, act, sides):
        now = cells.astype(F32)
        if act:
            now = silu(now)
        minus, plus = pltpu.roll(now, 1, 0), pltpu.roll(now, T - 1, 0)
        if sides:
            minus = jnp.where(edge == 0, hc32[0, pl.ds(i, 1), :], minus)
            plus = jnp.where(edge == T - 1, hc32[1, pl.ds(i, 1), :], plus)
        sh[0, i] = minus.astype(BF16)
        sh[1, i] = now.astype(BF16)
        sh[2, i] = plus.astype(BF16)

    def inner(sh, k, act, sides):
        @pl.loop(0, T, unroll=4)
        def _(i):
            emit(sh, i + 1, in4[k, i], act, sides)

    def outer(sh, k, act):
        emit(sh, 0, hrow[0, k], act, True)
        emit(sh, T + 1, hrow[1, k], act, True)

    def patch(sh):
        @pl.loop(1, T + 1, unroll=4)
        def _(i):
            cells = sh[0, i, 0:16, :].astype(F32)
            sh[0, i, 0:16, :] = jnp.where(half_edge == 0, hc32[0, pl.ds(i, 1), :], cells).astype(BF16)
            cells = sh[2, i, 16:32, :].astype(F32)
            sh[2, i, 16:32, :] = jnp.where(half_edge == 15, hc32[1, pl.ds(i, 1), :], cells).astype(BF16)

    def gather_rem(sh, rem):
        @pl.loop(0, 2)
        def _(n):
            span = pl.ds(n * 17, 17)
            parts = [sh[k, span].reshape(544, C)[:, 256:320] for k in range(3)]
            parts.append(jnp.zeros((544, 64), BF16))
            rem[span] = jnp.concatenate(parts, axis=1).reshape(17, T, 256)

    def arrange(w, slot):
        for a in range(3):
            for b in range(3):
                wrem[slot, a, :, (2 - b) * 64 : (3 - b) * 64] = w[a * 3 + b, :, 256:320]
                wn[slot, 2 - b, a * 64 : (a + 1) * 64, :] = w[a * 3 + b, 256:320, :256]
            wrem[slot, a, :, 192:256] = jnp.zeros((C, 64), BF16)
            wn[slot, 3, a * 64 : (a + 1) * 64, :] = wrem[slot, a, 256:320, :]
        wn[slot, :, 192:256, :] = jnp.zeros((4, 64, 256), BF16)

    def conv_tails(slot):
        @pl.loop(0, 2)
        def _(h):
            span = pl.ds(h * 17, 17)
            total = dot(remg[span].reshape(544, 256), wn[slot, 3], NT)
            for s in range(3):
                total += dot(shg[s, span].reshape(544, C)[:, :256], wn[slot, s], NT)
            tails[span] = total.reshape(17, T, 256)

    def conv(w, slot):
        parts = []
        for a in range(3):
            span = pl.ds(2 - a, T)
            for k in range(3):
                parts.append((shg[k, span].reshape(1024, C)[:, :256], w[a * 3 + 2 - k, :256, :256]))
            parts.append((remg[span].reshape(1024, 256), wrem[slot, a, :256, :]))
        total = dot(*parts[0], NT)
        for part in parts[1:]:
            total += dot(*part, NT)
        acc[...] = total

    def scaled(dst, rate):
        @pl.loop(0, 4)
        def _(h):
            span = pl.ds(h * 256, 256)
            dst[span, 0:256] = (rate[span, 0:256] * acc[span, :]).astype(BF16)
            last = (
                tails[pl.ds(h * 8 + 2, 8)].reshape(256, 256)[:, :64]
                + tails[pl.ds(h * 8 + 1, 8)].reshape(256, 256)[:, 64:128]
                + tails[pl.ds(h * 8, 8)].reshape(256, 256)[:, 128:192]
            )
            dst[span, 256:320] = (rate[span, 256:320] * last).astype(BF16)

    def slopes(dst, read):
        @pl.loop(0, T, unroll=4)
        def _(i):
            dst[pl.ds(pl.multiple_of(i * T, T), T), :] = slope(read(i).astype(F32))

    def turned(src):
        for n in range(4):
            gt[:, n * 256 : (n + 1) * 256] = dot(omat[...], src[n * 256 : (n + 1) * 256, :], NT).astype(BF16)

    def halves(dst, base, lane, width, value):
        value = value.astype(BF16)
        for half in range(2):
            dst[half, base : base + 160, lane : lane + width] = value[half * 160 : (half + 1) * 160]

    def weights(dst, base, sh, rem, a):
        span = pl.ds(a, T)
        for s in range(3):
            halves(dst, base, s * 256, 256, dot(gt[...], sh[s, span].reshape(1024, C)[:, :256]))
        halves(dst, base, 768, 256, dot(gt[...], rem[span].reshape(1024, 256)))

    def sides(n):
        scol[0, n] = in4[n, :, 0, :]
        scol[1, n] = in4[n, :, T - 1, :]

    loads[0].wait()
    for copy in loads[1:]:
        copy.start()
    sides(0)

    loads[1].wait()
    loads[2].wait()
    sides(1)
    sides(2)
    inner(shg, 0, False, False)
    slopes(rate2, lambda i: in4[1, i])

    count = jnp.int32(len(peers))
    for d in around:
        count = count + there[d].astype(jnp.int32)
    pl.semaphore_wait(barrier, count)

    def halo(first, size, phase):
        copies = []
        for n, (dr, dc) in enumerate(around):
            span = pl.ds(first, size)
            if dc == 0:
                src = in4.at[span, 0 if dr < 0 else T - 1]
                dst = hrow.at[1 if dr < 0 else 0, span]
            elif dr == 0:
                src = scol.at[0 if dc < 0 else 1, span]
                dst = hcol.at[1 if dc < 0 else 0, span]
            else:
                src = scol.at[0 if dc < 0 else 1, span, pl.ds(0 if dr < 0 else 16, 16)]
                dst = hcor.at[(1 if dr < 0 else 0) * 2 + (1 if dc < 0 else 0), span]
            copies.append(
                (
                    (dr, dc),
                    pltpu.make_async_remote_copy(
                        src_ref=src, dst_ref=dst,
                        send_sem=hs_sem.at[phase, n], recv_sem=hr_sem.at[phase, n],
                        device_id=(row + dr, col + dc), device_id_type=MESH,
                    ),
                )
            )
        return copies

    def start(copies):
        for d, copy in copies:
            pl.when(there[d])(copy.start)

    def finished(copies):
        for d, copy in copies:
            pl.when(there[d])(copy.wait_send)

    def landed(copies):
        for d, copy in copies:
            pl.when(there[(-d[0], -d[1])])(copy.wait_recv)

    first = halo(0, 1, 0)
    start(first)
    acts = halo(1, 2, 1)
    start(acts)

    def clear(condition, ref, slot):
        @pl.when(condition)
        def _():
            ref[slot] = jnp.zeros(ref.shape[1:], BF16)

    clear(row == 0, hrow, 0)
    clear(row == 15, hrow, 1)
    clear(col == 0, hcol, 0)
    clear(col == 15, hcol, 1)
    for slot in range(4):
        edge_row = row == (0 if slot < 2 else 15)
        edge_col = col == (0 if slot % 2 == 0 else 15)
        clear(jnp.logical_or(edge_row, edge_col), hcor, slot)

    counter = [0]

    def remote(src, dst, peer):
        n = counter[0]
        counter[0] += 1
        return pltpu.make_async_remote_copy(
            src_ref=src, dst_ref=dst, send_sem=send_sem.at[n], recv_sem=recv_sem.at[n],
            device_id=peer, device_id_type=MESH,
        )

    class Stage:
        def __init__(self, source, groups, rows, split, mine):
            self.source, self.groups, self.rows, self.split = source, groups, rows, split
            (self.landing, self.d, self.ha, self.hb, self.pa, self.pb,
             self.e, self.f, self.ea, self.fb) = mine
            self.sent = []

        def go(self, *copies):
            for copy in copies:
                copy.start()
            self.sent += copies
            return copies

        def drain(self):
            for copy in self.sent:
                copy.wait_send()
            self.sent = []

        def one(self):
            self.k1 = self.go(remote(self.source.at[1 - core], self.landing, partner))

        def put(self, base, yy, value):
            value = value.astype(BF16)
            for q in range(2):
                for h in range(2):
                    self.d[yy, h * 2 + q, pl.ds(base, 80), :] = value[
                        q * 80 : (q + 1) * 80, h * 128 : (h + 1) * 128
                    ]

        def two(self):
            for copy in self.k1:
                copy.wait_recv()

            def both(span, lanes):
                here = self.source[core, span, lanes].astype(F32)
                return (here + self.landing[span, lanes].astype(F32)).astype(BF16)

            for g in range(self.groups):
                span = slice(g * 160, (g + 1) * 160)
                parts = [both(span, slice(s * 256, (s + 1) * 256)) for s in range(4)]
                for yy in range(4):
                    total = dot(parts[0], pmat[yy * 3])
                    for s in range(1, 3):
                        total += dot(parts[s], pmat[yy * 3 + s])
                    if yy == 3:
                        total += dot(parts[3], pmat[12])
                    self.put(g * 80, yy, total)
            if self.groups == 0:
                main, last = (both(slice(0, 160), lanes) for lanes in (slice(0, 256), slice(256, 320)))
                for yy in range(4):
                    total = dot(main, pmat[yy * 3])
                    if yy == 3:
                        total += dot(last, pmat[12, 0:64])
                    self.put(0, yy, total)

            lo, hi = pl.ds(0, self.split), pl.ds(self.split, self.rows - self.split)
            far_y, far_x = (y + 2) % 4, (x + 2) % 4
            up_y, down_y, up_x, down_x = (y + 1) % 4, (y + 3) % 4, (x + 1) % 4, (x + 3) % 4
            low, high = pl.ds(0, 2), pl.ds(2, 2)
            self.k2 = self.go(
                remote(self.d.at[far_y, low, lo], self.ha.at[0], at_y(up_y)),
                remote(self.d.at[far_y, high, lo], self.ha.at[1], at_y(down_y)),
                remote(self.d.at[low, far_x, hi], self.hb.at[0], at_x(up_x)),
                remote(self.d.at[high, far_x, hi], self.hb.at[1], at_x(down_x)),
            )

        def relay(self):
            for copy in self.k2:
                copy.wait_recv()
            lo, hi = pl.ds(0, self.split), pl.ds(self.split, self.rows - self.split)
            for n in range(2):
                ty, tx = (y + 1 + 2 * n) % 4, (x + 1 + 2 * n) % 4
                for u in range(2):
                    t = 2 * n + u
                    self.d[ty, t, lo] = (self.d[ty, t, lo].astype(F32) + self.ha[n, u].astype(F32)).astype(BF16)
                    self.d[t, tx, hi] = (self.d[t, tx, hi].astype(F32) + self.hb[n, u].astype(F32)).astype(BF16)
            self.k3 = []
            for n in range(2):
                ty, tx = (y + 1 + 2 * n) % 4, (x + 1 + 2 * n) % 4
                self.k3 += self.go(
                    remote(self.d.at[ty, :, lo], self.pa.at[n], at_y(ty)),
                    remote(self.d.at[:, tx, hi], self.pb.at[n], at_x(tx)),
                )

        def three(self):
            for copy in self.k3:
                copy.wait_recv()
            lo, hi = pl.ds(0, self.split), pl.ds(self.split, self.rows - self.split)
            for t in range(4):
                total = self.d[y, t, lo].astype(F32) + self.pa[0, t].astype(F32) + self.pa[1, t].astype(F32)
                self.e[t] = total.astype(BF16)
                total = self.d[t, x, hi].astype(F32) + self.pb[0, t].astype(F32) + self.pb[1, t].astype(F32)
                self.f[t] = total.astype(BF16)
            self.k4 = []
            for d in (2, 1, 3):
                ty, tx = (y + d) % 4, (x + d) % 4
                self.k4 += self.go(
                    remote(self.e.at[tx], self.ea.at[d - 1], at_x(tx)),
                    remote(self.f.at[ty], self.fb.at[d - 1], at_y(ty)),
                )

        def collect(self, j, base):
            for copy in self.k4:
                copy.wait_recv()
            total = self.e[x].astype(F32)
            for d in range(3):
                total += self.ea[d].astype(F32)
            j[base : base + self.split] = total.astype(BF16)
            total = self.f[y].astype(F32)
            for d in range(3):
                total += self.fb[d].astype(F32)
            j[base + self.split : base + self.rows] = total.astype(BF16)

    class Last(Stage):
        def __init__(self, out, table, zn, rows, parts, mine):
            self.out, self.table, self.zn, self.rows, self.parts = out, table, zn, rows, parts
            self.j, self.zs, self.zr, self.fin, self.pin = mine
            self.sent = []

        def four(self):
            base = 0
            for part in self.parts:
                part.collect(self.j, base)
                base += part.rows
            pick = jnp.where(
                lax.broadcasted_iota(jnp.int32, (8 * self.zn, self.rows), 1) == self.table[...], 1.0, 0.0
            ).astype(BF16)
            self.zs[...] = dot(pick, self.j[...]).astype(BF16).reshape(8, self.zn, 128)
            self.k5 = []
            for d in (4, 3, 5, 2, 6, 1, 7):
                tz = (z + d) % 8
                self.k5 += self.go(remote(self.zs.at[tz], self.zr.at[d - 1], at_z(tz)))

        def five(self):
            for copy in self.k5:
                copy.wait_recv()
            total = self.zs[z].astype(F32)
            for d in range(7):
                total += self.zr[d].astype(F32)
            self.fin[...] = total
            self.k6 = self.go(remote(self.fin, self.pin, partner))
            self.show(core, total)

        def show(self, side, value):
            self.out[side] = jnp.where(core == 0, value[:, :64], value[:, 64:])

        def six(self):
            self.k6[0].wait_recv()
            self.show(1 - core, self.pin[...])

    stage_a = Stage(ra, 3, 240, 128, bufs[0:10])
    stage_b1 = Stage(rb1, 2, 160, 80, bufs[10:20])
    stage_b2 = Stage(rb2, 1, 80, 48, bufs[20:30])
    stage_c = Stage(rz, 0, 80, 48, bufs[30:40])
    last_a = Last(out_a, deal, ZN, 240, (stage_a,), bufs[40:45])
    last_b = Last(out_b, deal, ZN, 240, (stage_b1, stage_b2), bufs[45:50])
    last_c = Last(out_c, deal_c, ZC, 80, (stage_c,), bufs[50:55])

    loads[3].wait()
    arrange(wd, 0)
    loads[4].wait()
    slopes(rate1, lambda i: pre[i])
    loads[8].wait()
    omat[...] = jnp.where(
        lax.broadcasted_iota(jnp.int32, (C, C), 1) == order_ref[...], 1.0, 0.0
    ).astype(BF16)
    for n in range(9, 12):
        loads[n].wait()
    depth = lax.broadcasted_iota(jnp.int32, (256, 256), 0)

    @pl.loop(0, 13)
    def _(k):
        pmat[k] = jnp.where(depth == place_ref[pl.ds(k, 1), :], 1.0, 0.0).astype(BF16)

    loads[6].wait()
    arrange(wc, 1)
    landed(first)
    columns(0, False)
    outer(shg, 0, False)
    patch(shg)
    gather_rem(shg, remg)
    conv_tails(0)
    conv(wd, 0)
    scaled(dec, rate1)
    loads[5].wait()
    in4[3] = dot(dec[...], wz[...], NT).astype(BF16).reshape(T, T, C)
    sides(3)
    second = halo(3, 1, 2)
    start(second)

    landed(acts)
    columns(1, True)
    inner(shm, 1, True, True)
    outer(shm, 1, True)
    gather_rem(shm, remm)
    turned(in4[3].reshape(1024, C))
    for a in range(3):
        weights(ra, a * 160, shm, remm, a)
    stage_a.one()
    loads[7].wait()
    turned(dec)
    halves(rz, 0, 0, C, dot(gt[...], cout[...].reshape(1024, C)))
    stage_c.one()
    inner(shg, 3, False, False)
    landed(second)
    columns(3, False)
    outer(shg, 3, False)
    patch(shg)
    gather_rem(shg, remg)
    stage_a.two()
    stage_c.two()
    columns(2, True)
    inner(shi, 2, True, True)
    outer(shi, 2, True)
    gather_rem(shi, remi)
    conv_tails(1)
    conv(wc, 1)
    stage_a.relay()
    stage_c.relay()
    scaled(mgrad, rate2)
    turned(mgrad)
    for a in range(2):
        weights(rb1, a * 160, shi, remi, a)
    stage_b1.one()
    weights(rb2, 0, shi, remi, 2)
    stage_b2.one()
    stage_b1.two()
    stage_b2.two()
    stage_a.three()
    stage_c.three()
    stage_b1.relay()
    stage_b2.relay()
    last_a.four()
    last_c.four()
    stage_b1.three()
    stage_b2.three()
    last_b.four()
    last_a.five()
    last_c.five()
    last_a.six()
    last_c.six()
    finished(first)
    finished(acts)
    finished(second)
    for part in (stage_a, stage_b1, stage_b2, stage_c, last_a, last_b, last_c):
        part.drain()
    last_b.five()
    last_b.six()
    last_b.drain()


def finish(a_ref, b_ref, c_ref, zero_ref, ctrl_ref, in_ref):
    def exact(a, b, dims):
        return lax.dot_general(a, b, dims, precision=lax.Precision.HIGHEST, preferred_element_type=F32)

    r = lax.broadcasted_iota(jnp.int32, (72, 64), 0)
    lane = lax.broadcasted_iota(jnp.int32, (72, 64), 1)
    sel = jnp.zeros((72, 64), F32)
    for s in range(3):
        inside = (r >= s * 24) & (r < s * 24 + 20)
        sel = jnp.where(inside & (lane - s * 20 == r - s * 24), 1.0, sel)
    for ref, groups, dst in ((a_ref, 3, ctrl_ref), (b_ref, 3, in_ref), (c_ref, 1, None)):
        zn = ref.shape[1]
        turn = exact(sel, ref[...].reshape(2 * zn, 64), NT)
        k = lax.broadcasted_iota(jnp.int32, (2 * zn, 20), 0)
        n = lax.broadcasted_iota(jnp.int32, (2 * zn, 20), 1)
        for g in range(groups):
            pick = jnp.where(k == jnp.where(n < 10, n, n - 10 + zn) + g * 10, 1.0, 0.0)
            value = exact(turn, pick, NN)
            if dst is None:
                zero_ref[...] = value[0:20]
            else:
                for s in range(3):
                    dst[g * 3 + s] = value[s * 24 : s * 24 + 20]


def stage_buffers(landing, rows, split):
    rest = rows - split
    return [
        pltpu.VMEM(landing, BF16),
        pltpu.VMEM((4, 4, rows, 128), BF16),
        pltpu.VMEM((2, 2, split, 128), BF16),
        pltpu.VMEM((2, 2, rest, 128), BF16),
        pltpu.VMEM((2, 4, split, 128), BF16),
        pltpu.VMEM((2, 4, rest, 128), BF16),
        pltpu.VMEM((4, split, 128), BF16),
        pltpu.VMEM((4, rest, 128), BF16),
        pltpu.VMEM((3, split, 128), BF16),
        pltpu.VMEM((3, rest, 128), BF16),
    ]


def last_buffers(rows, zn):
    return [
        pltpu.VMEM((rows, 128), BF16),
        pltpu.VMEM((8, zn, 128), BF16),
        pltpu.VMEM((7, zn, 128), BF16),
        pltpu.VMEM((zn, 128), F32),
        pltpu.VMEM((zn, 128), F32),
    ]


def on_device(grad_out, dec_pre, ctrl_out, ctrl_mid, ctrl_in, dec_weight, zero_weight, ctrl_weight):
    tabs = [jnp.asarray(t) for t in tables()]
    anys = pl.BlockSpec(memory_space=pl.ANY)
    vmem = pl.BlockSpec(memory_space=pltpu.VMEM)
    shifts = [pltpu.VMEM((3, T + 2, T, C), BF16), pltpu.VMEM((T + 2, T, 256), BF16)]
    blocks = pl.pallas_call(
        kernel,
        out_shape=[jax.ShapeDtypeStruct((2, zn, 64), F32) for zn in (ZN, ZN, ZC)],
        in_specs=[anys] * 12,
        out_specs=[vmem] * 3,
        scratch_shapes=[
            *[pltpu.VMEM(t.shape, jnp.int32) for t in tabs],
            pltpu.VMEM((4, T, T, C), BF16),
            pltpu.VMEM((T, T, C), BF16),
            pltpu.VMEM((T, T, C), BF16),
            pltpu.VMEM((9, C, C), BF16),
            pltpu.VMEM((C, C), BF16),
            pltpu.VMEM((9, C, C), BF16),
            pltpu.VMEM((2, 4, T, C), BF16),
            pltpu.VMEM((2, 4, T, C), BF16),
            pltpu.VMEM((2, 4, T, C), BF16),
            pltpu.VMEM((4, 4, 16, C), BF16),
            pltpu.VMEM((2, 40, C), F32),
            *shifts, *shifts, *shifts,
            pltpu.VMEM((2, 3, C, 256), BF16),
            pltpu.VMEM((2, 4, 256, 256), BF16),
            pltpu.VMEM((T + 2, T, 256), F32),
            pltpu.VMEM((1024, 256), F32),
            pltpu.VMEM((1024, C), F32),
            pltpu.VMEM((1024, C), F32),
            pltpu.VMEM((1024, C), BF16),
            pltpu.VMEM((13, 256, 256), BF16),
            pltpu.VMEM((C, C), BF16),
            pltpu.VMEM((C, 1024), BF16),
            pltpu.VMEM((1024, C), BF16),
            pltpu.VMEM((2, 480, 1024), BF16),
            pltpu.VMEM((2, 160, C), BF16),
            pltpu.VMEM((2, 320, 1024), BF16),
            pltpu.VMEM((2, 160, 1024), BF16),
        ]
        + stage_buffers((480, 1024), 240, 128)
        + stage_buffers((320, 1024), 160, 80)
        + stage_buffers((160, 1024), 80, 48)
        + stage_buffers((160, C), 80, 48)
        + last_buffers(240, ZN)
        + last_buffers(240, ZN)
        + last_buffers(80, ZC)
        + [
            pltpu.SemaphoreType.DMA((12,)),
            pltpu.SemaphoreType.DMA((3, 8)),
            pltpu.SemaphoreType.DMA((3, 8)),
            pltpu.SemaphoreType.DMA((N_SEM,)),
            pltpu.SemaphoreType.DMA((N_SEM,)),
        ],
        compiler_params=pltpu.CompilerParams(
            collective_id=0, has_side_effects=True, vmem_limit_bytes=60 * 1024 * 1024
        ),
        name="fused",
    )(
        grad_out, dec_pre, ctrl_out, ctrl_mid, ctrl_in,
        dec_weight.reshape(9, C, C), zero_weight, ctrl_weight.reshape(9, C, C), *tabs,
    )

    grad_zero, grad_ctrl, grad_in = pl.pallas_call(
        finish,
        out_shape=[
            jax.ShapeDtypeStruct((20, 20), F32),
            jax.ShapeDtypeStruct((9, 20, 20), F32),
            jax.ShapeDtypeStruct((9, 20, 20), F32),
        ],
        in_specs=[vmem] * 3,
        out_specs=[vmem] * 3,
        name="finish",
    )(*blocks)
    return (grad_zero, grad_ctrl.reshape(3, 3, 20, 20), grad_in.reshape(3, 3, 20, 20))


def solution(mesh):
    tile = P("row", "col", None)
    return jax.shard_map(
        on_device,
        mesh=mesh,
        in_specs=(tile,) * 5 + (P(),) * 3,
        out_specs=(P("row", "col"), P(None, None, "row", "col"), P(None, None, "row", "col")),
        check_vma=False,
    )
```

```python
import jax
import jax.numpy as jnp
import numpy as np
from jax import lax
from jax.experimental import pallas as pl
from jax.experimental.pallas import tpu as pltpu
from jax.sharding import PartitionSpec as P

F32 = jnp.float32
BF16 = jnp.bfloat16
MESH = pl.DeviceIdType.MESH
NT = (((1,), (1,)), ((), ()))
NN = (((1,), (0,)), ((), ()))
C = 320
T = 32
ZN, ZC = 32, 16
N_SEM = 96


def dot(a, b, dims=NN):
    return lax.dot_general(a, b, dims, preferred_element_type=F32)


def silu(v):
    return v * jax.nn.sigmoid(v)


def slope(v):
    s = jax.nn.sigmoid(v)
    return s * (1.0 + v * (1.0 - s))


def tables():
    place = np.full((16, 256), -1, np.int32)
    for y in range(4):
        for s in range(3):
            for xh in range(2):
                for core in range(2):
                    for i in range(20):
                        lane = xh * 128 + core * 64 + s * 20 + i
                        c = y * 80 + xh * 40 + core * 20 + i
                        if c < 256:
                            place[y * 3 + s, lane] = c
                        else:
                            place[12, lane] = s * 64 + c - 256
    order = np.zeros((C, 1), np.int32)
    for core in range(2):
        for xl in range(2):
            for z in range(8):
                for i in range(10):
                    order[core * 160 + xl * 80 + z * 10 + i, 0] = (xl * 8 + z) * 20 + core * 10 + i
    deals = []
    for zn, groups in ((ZN, 3), (ZC, 1)):
        deal = np.full((8 * zn, 1), -1, np.int32)
        for z in range(8):
            for g in range(groups):
                for i in range(10):
                    deal[z * zn + g * 10 + i, 0] = g * 80 + z * 10 + i
        deals.append(deal)
    return place, order, *deals


def kernel(
    g_hbm, pre_hbm, cout_hbm, mid_hbm, cin_hbm, wd_hbm, wz_hbm, wc_hbm,
    place_hbm, order_hbm, deal_hbm, deal_c_hbm,
    out_a, out_b, out_c,
    place_ref, order_ref, deal, deal_c,
    in4, pre, cout, wd, wz, wc,
    scol, hrow, hcol, hcor, hc32,
    shg, remg, shm, remm, shi, remi,
    wrem, wn, tails, acc, rate1, rate2, dec, pmat, omat, gt, mgrad,
    ra, rz, rb1, rb2, picks, picks_c,
    *rest,
):
    bufs, (load_sem, hs_sem, hr_sem, send_sem, recv_sem) = rest[:-5], rest[-5:]
    row = lax.axis_index("row")
    col = lax.axis_index("col")
    y, xh, core = row // 4, (row // 2) % 2, row % 2
    xl, z = col // 8, col % 8
    x = xh * 2 + xl

    def at_y(t):
        return ((t * 2 + xh) * 2 + core, col)

    def at_x(t):
        return ((y * 2 + t // 2) * 2 + core, (t % 2) * 8 + z)

    def at_z(t):
        return (row, xl * 8 + t)

    partner = (row + 1 - 2 * core, col)

    loads = [
        pltpu.make_async_copy(g_hbm, in4.at[0], load_sem.at[0]),
        pltpu.make_async_copy(mid_hbm, in4.at[1], load_sem.at[1]),
        pltpu.make_async_copy(cin_hbm, in4.at[2], load_sem.at[2]),
        pltpu.make_async_copy(wd_hbm, wd, load_sem.at[3]),
        pltpu.make_async_copy(pre_hbm, pre, load_sem.at[4]),
        pltpu.make_async_copy(wz_hbm, wz, load_sem.at[5]),
        pltpu.make_async_copy(wc_hbm, wc, load_sem.at[6]),
        pltpu.make_async_copy(cout_hbm, cout, load_sem.at[7]),
        pltpu.make_async_copy(order_hbm, order_ref, load_sem.at[8]),
        pltpu.make_async_copy(place_hbm, place_ref, load_sem.at[9]),
        pltpu.make_async_copy(deal_hbm, deal, load_sem.at[10]),
        pltpu.make_async_copy(deal_c_hbm, deal_c, load_sem.at[11]),
    ]
    loads[0].start()

    has = {-1: (row > 0, col > 0), 1: (row < 15, col < 15), 0: (row >= 0, col >= 0)}
    around = [(dr, dc) for dr in (-1, 0, 1) for dc in (-1, 0, 1) if (dr, dc) != (0, 0)]
    there = {d: jnp.logical_and(has[d[0]][0], has[d[1]][1]) for d in around}

    barrier = pltpu.get_barrier_semaphore()
    for d in around:
        @pl.when(there[d])
        def _(d=d):
            pl.semaphore_signal(barrier, inc=1, device_id=(row + d[0], col + d[1]), device_id_type=MESH)
    peers = [partner]
    peers += [at_y((y + d) % 4) for d in range(1, 4)]
    peers += [at_x((x + d) % 4) for d in range(1, 4)]
    peers += [at_z((z + d) % 8) for d in range(1, 8)]
    for peer in peers:
        pl.semaphore_signal(barrier, inc=1, device_id=peer, device_id_type=MESH)

    edge = lax.broadcasted_iota(jnp.int32, (T, C), 0)
    half_edge = lax.broadcasted_iota(jnp.int32, (16, C), 0)

    def columns(k, act):
        for side in range(2):
            parts = (hcor[side, k].astype(F32), hcol[side, k].astype(F32), hcor[2 + side, k].astype(F32))
            if act:
                parts = [silu(v) for v in parts]
            hc32[side, 0:1, :] = parts[0][15:16]
            hc32[side, 1:33, :] = parts[1]
            hc32[side, 33:34, :] = parts[2][0:1]

    def emit(sh, i, cells, act, sides):
        now = cells.astype(F32)
        if act:
            now = silu(now)
        minus, plus = pltpu.roll(now, 1, 0), pltpu.roll(now, T - 1, 0)
        if sides:
            minus = jnp.where(edge == 0, hc32[0, pl.ds(i, 1), :], minus)
            plus = jnp.where(edge == T - 1, hc32[1, pl.ds(i, 1), :], plus)
        sh[0, i] = minus.astype(BF16)
        sh[1, i] = now.astype(BF16)
        sh[2, i] = plus.astype(BF16)

    def inner(sh, k, act, sides):
        @pl.loop(0, T, unroll=4)
        def _(i):
            emit(sh, i + 1, in4[k, i], act, sides)

    def outer(sh, k, act):
        emit(sh, 0, hrow[0, k], act, True)
        emit(sh, T + 1, hrow[1, k], act, True)

    def patch(sh):
        @pl.loop(1, T + 1, unroll=4)
        def _(i):
            cells = sh[0, i, 0:16, :].astype(F32)
            sh[0, i, 0:16, :] = jnp.where(half_edge == 0, hc32[0, pl.ds(i, 1), :], cells).astype(BF16)
            cells = sh[2, i, 16:32, :].astype(F32)
            sh[2, i, 16:32, :] = jnp.where(half_edge == 15, hc32[1, pl.ds(i, 1), :], cells).astype(BF16)

    def gather_rem(sh, rem):
        @pl.loop(0, 2)
        def _(n):
            span = pl.ds(n * 17, 17)
            parts = [sh[k, span].reshape(544, C)[:, 256:320] for k in range(3)]
            parts.append(jnp.zeros((544, 64), BF16))
            rem[span] = jnp.concatenate(parts, axis=1).reshape(17, T, 256)

    def arrange(w, slot):
        for a in range(3):
            for b in range(3):
                wrem[slot, a, :, (2 - b) * 64 : (3 - b) * 64] = w[a * 3 + b, :, 256:320]
                wn[slot, 2 - b, a * 64 : (a + 1) * 64, :] = w[a * 3 + b, 256:320, :256]
            wrem[slot, a, :, 192:256] = jnp.zeros((C, 64), BF16)
            wn[slot, 3, a * 64 : (a + 1) * 64, :] = wrem[slot, a, 256:320, :]
        wn[slot, :, 192:256, :] = jnp.zeros((4, 64, 256), BF16)

    def conv_tails(slot):
        @pl.loop(0, 2)
        def _(h):
            span = pl.ds(h * 17, 17)
            total = dot(remg[span].reshape(544, 256), wn[slot, 3], NT)
            for s in range(3):
                total += dot(shg[s, span].reshape(544, C)[:, :256], wn[slot, s], NT)
            tails[span] = total.reshape(17, T, 256)

    def conv(w, slot):
        parts = []
        for a in range(3):
            span = pl.ds(2 - a, T)
            for k in range(3):
                parts.append((shg[k, span].reshape(1024, C)[:, :256], w[a * 3 + 2 - k, :256, :256]))
            parts.append((remg[span].reshape(1024, 256), wrem[slot, a, :256, :]))
        total = dot(*parts[0], NT)
        for part in parts[1:]:
            total += dot(*part, NT)
        acc[...] = total

    def scaled(dst, rate):
        @pl.loop(0, 4)
        def _(h):
            span = pl.ds(h * 256, 256)
            dst[span, 0:256] = (rate[span, 0:256] * acc[span, :]).astype(BF16)
            last = (
                tails[pl.ds(h * 8 + 2, 8)].reshape(256, 256)[:, :64]
                + tails[pl.ds(h * 8 + 1, 8)].reshape(256, 256)[:, 64:128]
                + tails[pl.ds(h * 8, 8)].reshape(256, 256)[:, 128:192]
            )
            dst[span, 256:320] = (rate[span, 256:320] * last).astype(BF16)

    def slopes(dst, read):
        @pl.loop(0, T, unroll=4)
        def _(i):
            dst[pl.ds(pl.multiple_of(i * T, T), T), :] = slope(read(i).astype(F32))

    def turned(src):
        for n in range(4):
            gt[:, n * 256 : (n + 1) * 256] = dot(omat[...], src[n * 256 : (n + 1) * 256, :], NT).astype(BF16)

    def halves(dst, base, lane, width, value):
        value = value.astype(BF16)
        for half in range(2):
            dst[half, base : base + 160, lane : lane + width] = value[half * 160 : (half + 1) * 160]

    def weights(dst, base, sh, rem, a):
        span = pl.ds(a, T)
        for s in range(3):
            halves(dst, base, s * 256, 256, dot(gt[...], sh[s, span].reshape(1024, C)[:, :256]))
        halves(dst, base, 768, 256, dot(gt[...], rem[span].reshape(1024, 256)))

    def sides(n):
        scol[0, n] = in4[n, :, 0, :]
        scol[1, n] = in4[n, :, T - 1, :]

    loads[0].wait()
    for copy in loads[1:]:
        copy.start()
    sides(0)

    loads[1].wait()
    loads[2].wait()
    sides(1)
    sides(2)
    inner(shg, 0, False, False)
    slopes(rate2, lambda i: in4[1, i])

    count = jnp.int32(len(peers))
    for d in around:
        count = count + there[d].astype(jnp.int32)
    pl.semaphore_wait(barrier, count)

    def halo(first, size, phase):
        copies = []
        for n, (dr, dc) in enumerate(around):
            span = pl.ds(first, size)
            if dc == 0:
                src = in4.at[span, 0 if dr < 0 else T - 1]
                dst = hrow.at[1 if dr < 0 else 0, span]
            elif dr == 0:
                src = scol.at[0 if dc < 0 else 1, span]
                dst = hcol.at[1 if dc < 0 else 0, span]
            else:
                src = scol.at[0 if dc < 0 else 1, span, pl.ds(0 if dr < 0 else 16, 16)]
                dst = hcor.at[(1 if dr < 0 else 0) * 2 + (1 if dc < 0 else 0), span]
            copies.append(
                (
                    (dr, dc),
                    pltpu.make_async_remote_copy(
                        src_ref=src, dst_ref=dst,
                        send_sem=hs_sem.at[phase, n], recv_sem=hr_sem.at[phase, n],
                        device_id=(row + dr, col + dc), device_id_type=MESH,
                    ),
                )
            )
        return copies

    def start(copies):
        for d, copy in copies:
            pl.when(there[d])(copy.start)

    def finished(copies):
        for d, copy in copies:
            pl.when(there[d])(copy.wait_send)

    def landed(copies):
        for d, copy in copies:
            pl.when(there[(-d[0], -d[1])])(copy.wait_recv)

    first = halo(0, 1, 0)
    start(first)
    acts = halo(1, 2, 1)
    start(acts)

    def clear(condition, ref, slot):
        @pl.when(condition)
        def _():
            ref[slot] = jnp.zeros(ref.shape[1:], BF16)

    clear(row == 0, hrow, 0)
    clear(row == 15, hrow, 1)
    clear(col == 0, hcol, 0)
    clear(col == 15, hcol, 1)
    for slot in range(4):
        edge_row = row == (0 if slot < 2 else 15)
        edge_col = col == (0 if slot % 2 == 0 else 15)
        clear(jnp.logical_or(edge_row, edge_col), hcor, slot)

    counter = [0]

    def remote(src, dst, peer):
        n = counter[0]
        counter[0] += 1
        return pltpu.make_async_remote_copy(
            src_ref=src, dst_ref=dst, send_sem=send_sem.at[n], recv_sem=recv_sem.at[n],
            device_id=peer, device_id_type=MESH,
        )

    class Stage:
        def __init__(self, source, groups, rows, split, mine):
            self.source, self.groups, self.rows, self.split = source, groups, rows, split
            (self.landing, self.d, self.ha, self.hb, self.pa, self.pb,
             self.e, self.f, self.ea, self.fb) = mine
            self.sent = []

        def go(self, *copies):
            for copy in copies:
                copy.start()
            self.sent += copies
            return copies

        def drain(self):
            for copy in self.sent:
                copy.wait_send()
            self.sent = []

        def one(self):
            self.k1 = self.go(remote(self.source.at[1 - core], self.landing, partner))

        def put(self, base, yy, value):
            value = value.astype(BF16)
            for q in range(2):
                for h in range(2):
                    self.d[yy, h * 2 + q, pl.ds(base, 80), :] = value[
                        q * 80 : (q + 1) * 80, h * 128 : (h + 1) * 128
                    ]

        def two(self):
            for copy in self.k1:
                copy.wait_recv()

            def both(span, lanes):
                here = self.source[core, span, lanes].astype(F32)
                return (here + self.landing[span, lanes].astype(F32)).astype(BF16)

            for g in range(self.groups):
                span = slice(g * 160, (g + 1) * 160)
                parts = [both(span, slice(s * 256, (s + 1) * 256)) for s in range(4)]
                for yy in range(4):
                    total = dot(parts[0], pmat[yy * 3])
                    for s in range(1, 3):
                        total += dot(parts[s], pmat[yy * 3 + s])
                    if yy == 3:
                        total += dot(parts[3], pmat[12])
                    self.put(g * 80, yy, total)
            if self.groups == 0:
                main, last = (both(slice(0, 160), lanes) for lanes in (slice(0, 256), slice(256, 320)))
                for yy in range(4):
                    total = dot(main, pmat[yy * 3])
                    if yy == 3:
                        total += dot(last, pmat[12, 0:64])
                    self.put(0, yy, total)

            lo, hi = pl.ds(0, self.split), pl.ds(self.split, self.rows - self.split)
            far_y, far_x = (y + 2) % 4, (x + 2) % 4
            up_y, down_y, up_x, down_x = (y + 1) % 4, (y + 3) % 4, (x + 1) % 4, (x + 3) % 4
            low, high = pl.ds(0, 2), pl.ds(2, 2)
            self.k2 = self.go(
                remote(self.d.at[far_y, low, lo], self.ha.at[0], at_y(up_y)),
                remote(self.d.at[far_y, high, lo], self.ha.at[1], at_y(down_y)),
                remote(self.d.at[low, far_x, hi], self.hb.at[0], at_x(up_x)),
                remote(self.d.at[high, far_x, hi], self.hb.at[1], at_x(down_x)),
            )

        def relay(self):
            for copy in self.k2:
                copy.wait_recv()
            lo, hi = pl.ds(0, self.split), pl.ds(self.split, self.rows - self.split)
            for n in range(2):
                ty, tx = (y + 1 + 2 * n) % 4, (x + 1 + 2 * n) % 4
                for u in range(2):
                    t = 2 * n + u
                    self.d[ty, t, lo] = (self.d[ty, t, lo].astype(F32) + self.ha[n, u].astype(F32)).astype(BF16)
                    self.d[t, tx, hi] = (self.d[t, tx, hi].astype(F32) + self.hb[n, u].astype(F32)).astype(BF16)
            self.k3 = []
            for n in range(2):
                ty, tx = (y + 1 + 2 * n) % 4, (x + 1 + 2 * n) % 4
                self.k3 += self.go(
                    remote(self.d.at[ty, :, lo], self.pa.at[n], at_y(ty)),
                    remote(self.d.at[:, tx, hi], self.pb.at[n], at_x(tx)),
                )

        def three(self):
            for copy in self.k3:
                copy.wait_recv()
            lo, hi = pl.ds(0, self.split), pl.ds(self.split, self.rows - self.split)
            for t in range(4):
                total = self.d[y, t, lo].astype(F32) + self.pa[0, t].astype(F32) + self.pa[1, t].astype(F32)
                self.e[t] = total.astype(BF16)
                total = self.d[t, x, hi].astype(F32) + self.pb[0, t].astype(F32) + self.pb[1, t].astype(F32)
                self.f[t] = total.astype(BF16)
            self.k4 = []
            for d in (2, 1, 3):
                ty, tx = (y + d) % 4, (x + d) % 4
                self.k4 += self.go(
                    remote(self.e.at[tx], self.ea.at[d - 1], at_x(tx)),
                    remote(self.f.at[ty], self.fb.at[d - 1], at_y(ty)),
                )

        def collect(self, j, base):
            for copy in self.k4:
                copy.wait_recv()
            total = self.e[x].astype(F32)
            for d in range(3):
                total += self.ea[d].astype(F32)
            j[base : base + self.split] = total.astype(BF16)
            total = self.f[y].astype(F32)
            for d in range(3):
                total += self.fb[d].astype(F32)
            j[base + self.split : base + self.rows] = total.astype(BF16)

    class Last(Stage):
        def __init__(self, out, pick, zn, parts, mine):
            self.out, self.pick, self.zn, self.parts = out, pick, zn, parts
            self.j, self.zs, self.zr, self.fin, self.pin = mine
            self.sent = []

        def four(self):
            base = 0
            for part in self.parts:
                part.collect(self.j, base)
                base += part.rows
            self.zs[...] = dot(self.pick[...], self.j[...]).astype(BF16).reshape(8, self.zn, 128)
            self.k5 = []
            for d in (4, 3, 5, 2, 6, 1, 7):
                tz = (z + d) % 8
                self.k5 += self.go(remote(self.zs.at[tz], self.zr.at[d - 1], at_z(tz)))

        def five(self):
            for copy in self.k5:
                copy.wait_recv()
            total = self.zs[z].astype(F32)
            for d in range(7):
                total += self.zr[d].astype(F32)
            self.fin[...] = total
            self.k6 = self.go(remote(self.fin, self.pin, partner))
            self.show(core, total)

        def show(self, side, value):
            self.out[side] = jnp.where(core == 0, value[:, :64], value[:, 64:])

        def six(self):
            self.k6[0].wait_recv()
            self.show(1 - core, self.pin[...])

    stage_a = Stage(ra, 3, 240, 128, bufs[0:10])
    stage_b1 = Stage(rb1, 2, 160, 80, bufs[10:20])
    stage_b2 = Stage(rb2, 1, 80, 48, bufs[20:30])
    stage_c = Stage(rz, 0, 80, 48, bufs[30:40])
    last_a = Last(out_a, picks, ZN, (stage_a,), bufs[40:45])
    last_b = Last(out_b, picks, ZN, (stage_b1, stage_b2), bufs[45:50])
    last_c = Last(out_c, picks_c, ZC, (stage_c,), bufs[50:55])

    loads[3].wait()
    arrange(wd, 0)
    loads[4].wait()
    slopes(rate1, lambda i: pre[i])
    loads[8].wait()
    omat[...] = jnp.where(
        lax.broadcasted_iota(jnp.int32, (C, C), 1) == order_ref[...], 1.0, 0.0
    ).astype(BF16)
    for n in range(9, 12):
        loads[n].wait()
    depth = lax.broadcasted_iota(jnp.int32, (256, 256), 0)

    @pl.loop(0, 13)
    def _(k):
        pmat[k] = jnp.where(depth == place_ref[pl.ds(k, 1), :], 1.0, 0.0).astype(BF16)

    loads[6].wait()
    arrange(wc, 1)
    inner(shm, 1, True, False)
    inner(shi, 2, True, False)
    for pick, table in ((picks, deal), (picks_c, deal_c)):
        pick[...] = jnp.where(
            lax.broadcasted_iota(jnp.int32, pick.shape, 1) == table[...], 1.0, 0.0
        ).astype(BF16)
    landed(first)
    columns(0, False)
    outer(shg, 0, False)
    patch(shg)
    gather_rem(shg, remg)
    conv_tails(0)
    conv(wd, 0)
    scaled(dec, rate1)
    loads[5].wait()
    in4[3] = dot(dec[...], wz[...], NT).astype(BF16).reshape(T, T, C)
    sides(3)
    second = halo(3, 1, 2)
    start(second)

    landed(acts)
    columns(1, True)
    outer(shm, 1, True)
    patch(shm)
    gather_rem(shm, remm)
    turned(in4[3].reshape(1024, C))
    for a in range(3):
        weights(ra, a * 160, shm, remm, a)
    stage_a.one()
    loads[7].wait()
    turned(dec)
    halves(rz, 0, 0, C, dot(gt[...], cout[...].reshape(1024, C)))
    stage_c.one()
    inner(shg, 3, False, False)
    landed(second)
    columns(3, False)
    outer(shg, 3, False)
    patch(shg)
    gather_rem(shg, remg)
    stage_a.two()
    stage_c.two()
    columns(2, True)
    outer(shi, 2, True)
    patch(shi)
    gather_rem(shi, remi)
    conv_tails(1)
    conv(wc, 1)
    stage_a.relay()
    stage_c.relay()
    scaled(mgrad, rate2)
    turned(mgrad)
    for a in range(2):
        weights(rb1, a * 160, shi, remi, a)
    stage_b1.one()
    weights(rb2, 0, shi, remi, 2)
    stage_b2.one()
    stage_b1.two()
    stage_b2.two()
    stage_a.three()
    stage_c.three()
    stage_b1.relay()
    stage_b2.relay()
    last_a.four()
    last_c.four()
    stage_b1.three()
    stage_b2.three()
    last_b.four()
    last_a.five()
    last_c.five()
    last_a.six()
    last_c.six()
    finished(first)
    finished(acts)
    finished(second)
    for part in (stage_a, stage_b1, stage_b2, stage_c, last_a, last_b, last_c):
        part.drain()
    last_b.five()
    last_b.six()
    last_b.drain()


def finish(a_ref, b_ref, c_ref, zero_ref, ctrl_ref, in_ref):
    def exact(a, b, dims):
        return lax.dot_general(a, b, dims, precision=lax.Precision.HIGHEST, preferred_element_type=F32)

    r = lax.broadcasted_iota(jnp.int32, (72, 64), 0)
    lane = lax.broadcasted_iota(jnp.int32, (72, 64), 1)
    sel = jnp.zeros((72, 64), F32)
    for s in range(3):
        inside = (r >= s * 24) & (r < s * 24 + 20)
        sel = jnp.where(inside & (lane - s * 20 == r - s * 24), 1.0, sel)
    for ref, groups, dst in ((a_ref, 3, ctrl_ref), (b_ref, 3, in_ref), (c_ref, 1, None)):
        zn = ref.shape[1]
        turn = exact(sel, ref[...].reshape(2 * zn, 64), NT)
        k = lax.broadcasted_iota(jnp.int32, (2 * zn, 20), 0)
        n = lax.broadcasted_iota(jnp.int32, (2 * zn, 20), 1)
        for g in range(groups):
            pick = jnp.where(k == jnp.where(n < 10, n, n - 10 + zn) + g * 10, 1.0, 0.0)
            value = exact(turn, pick, NN)
            if dst is None:
                zero_ref[...] = value[0:20]
            else:
                for s in range(3):
                    dst[g * 3 + s] = value[s * 24 : s * 24 + 20]


def stage_buffers(landing, rows, split):
    rest = rows - split
    return [
        pltpu.VMEM(landing, BF16),
        pltpu.VMEM((4, 4, rows, 128), BF16),
        pltpu.VMEM((2, 2, split, 128), BF16),
        pltpu.VMEM((2, 2, rest, 128), BF16),
        pltpu.VMEM((2, 4, split, 128), BF16),
        pltpu.VMEM((2, 4, rest, 128), BF16),
        pltpu.VMEM((4, split, 128), BF16),
        pltpu.VMEM((4, rest, 128), BF16),
        pltpu.VMEM((3, split, 128), BF16),
        pltpu.VMEM((3, rest, 128), BF16),
    ]


def last_buffers(rows, zn):
    return [
        pltpu.VMEM((rows, 128), BF16),
        pltpu.VMEM((8, zn, 128), BF16),
        pltpu.VMEM((7, zn, 128), BF16),
        pltpu.VMEM((zn, 128), F32),
        pltpu.VMEM((zn, 128), F32),
    ]


def on_device(grad_out, dec_pre, ctrl_out, ctrl_mid, ctrl_in, dec_weight, zero_weight, ctrl_weight):
    tabs = [jnp.asarray(t) for t in tables()]
    anys = pl.BlockSpec(memory_space=pl.ANY)
    vmem = pl.BlockSpec(memory_space=pltpu.VMEM)
    shifts = [pltpu.VMEM((3, T + 2, T, C), BF16), pltpu.VMEM((T + 2, T, 256), BF16)]
    blocks = pl.pallas_call(
        kernel,
        out_shape=[jax.ShapeDtypeStruct((2, zn, 64), F32) for zn in (ZN, ZN, ZC)],
        in_specs=[anys] * 12,
        out_specs=[vmem] * 3,
        scratch_shapes=[
            *[pltpu.VMEM(t.shape, jnp.int32) for t in tabs],
            pltpu.VMEM((4, T, T, C), BF16),
            pltpu.VMEM((T, T, C), BF16),
            pltpu.VMEM((T, T, C), BF16),
            pltpu.VMEM((9, C, C), BF16),
            pltpu.VMEM((C, C), BF16),
            pltpu.VMEM((9, C, C), BF16),
            pltpu.VMEM((2, 4, T, C), BF16),
            pltpu.VMEM((2, 4, T, C), BF16),
            pltpu.VMEM((2, 4, T, C), BF16),
            pltpu.VMEM((4, 4, 16, C), BF16),
            pltpu.VMEM((2, 40, C), F32),
            *shifts, *shifts, *shifts,
            pltpu.VMEM((2, 3, C, 256), BF16),
            pltpu.VMEM((2, 4, 256, 256), BF16),
            pltpu.VMEM((T + 2, T, 256), F32),
            pltpu.VMEM((1024, 256), F32),
            pltpu.VMEM((1024, C), F32),
            pltpu.VMEM((1024, C), F32),
            pltpu.VMEM((1024, C), BF16),
            pltpu.VMEM((13, 256, 256), BF16),
            pltpu.VMEM((C, C), BF16),
            pltpu.VMEM((C, 1024), BF16),
            pltpu.VMEM((1024, C), BF16),
            pltpu.VMEM((2, 480, 1024), BF16),
            pltpu.VMEM((2, 160, C), BF16),
            pltpu.VMEM((2, 320, 1024), BF16),
            pltpu.VMEM((2, 160, 1024), BF16),
            pltpu.VMEM((8 * ZN, 240), BF16),
            pltpu.VMEM((8 * ZC, 80), BF16),
        ]
        + stage_buffers((480, 1024), 240, 128)
        + stage_buffers((320, 1024), 160, 80)
        + stage_buffers((160, 1024), 80, 48)
        + stage_buffers((160, C), 80, 48)
        + last_buffers(240, ZN)
        + last_buffers(240, ZN)
        + last_buffers(80, ZC)
        + [
            pltpu.SemaphoreType.DMA((12,)),
            pltpu.SemaphoreType.DMA((3, 8)),
            pltpu.SemaphoreType.DMA((3, 8)),
            pltpu.SemaphoreType.DMA((N_SEM,)),
            pltpu.SemaphoreType.DMA((N_SEM,)),
        ],
        compiler_params=pltpu.CompilerParams(
            collective_id=0, has_side_effects=True, vmem_limit_bytes=60 * 1024 * 1024
        ),
        name="fused",
    )(
        grad_out, dec_pre, ctrl_out, ctrl_mid, ctrl_in,
        dec_weight.reshape(9, C, C), zero_weight, ctrl_weight.reshape(9, C, C), *tabs,
    )

    grad_zero, grad_ctrl, grad_in = pl.pallas_call(
        finish,
        out_shape=[
            jax.ShapeDtypeStruct((20, 20), F32),
            jax.ShapeDtypeStruct((9, 20, 20), F32),
            jax.ShapeDtypeStruct((9, 20, 20), F32),
        ],
        in_specs=[vmem] * 3,
        out_specs=[vmem] * 3,
        name="finish",
    )(*blocks)
    return (grad_zero, grad_ctrl.reshape(3, 3, 20, 20), grad_in.reshape(3, 3, 20, 20))


def solution(mesh):
    tile = P("row", "col", None)
    return jax.shard_map(
        on_device,
        mesh=mesh,
        in_specs=(tile,) * 5 + (P(),) * 3,
        out_specs=(P("row", "col"), P(None, None, "row", "col"), P(None, None, "row", "col")),
        check_vma=False,
    )
```
